32 devices in a mesh: tensor: 2 (over x), dp: 16 (over z, y, core).
Axes of the slice: x: 2, y: 2, z: 4, core: 2. Of those that a mesh axis runs over, the one named last changes fastest.
Arguments:
- tokens: bfloat16 [2048, 8192], P('dp', 'tensor'), may hold values from -6 to 6
- projection_weights: bfloat16 [2, 8192, 256], P(None, None, 'tensor'), may hold values from -0.0625 to 0.0625
- head_cotangent: bfloat16 [2, 2048, 256], P(None, 'dp', 'tensor'), may hold values from -6 to 6
- frequencies: int32 [2, 1024], replicated, may hold values from 0 to 8191, as said below
- sign_bits: int32 [2, 8192], replicated, may hold values 0 or 1
- first_moment: float32 [2, 1024, 256], P(None, 'dp', 'tensor'), may hold values from -6 to 6
- second_moment: float32 [2, 1024, 256], P(None, 'dp', 'tensor'), may hold values from 0.2 to 2
Outputs:
- input_gradient: bfloat16 [2048, 8192], P('dp', 'tensor')
- new_first: float32 [2, 1024, 256], P(None, 'dp', 'tensor')
- new_second: float32 [2, 1024, 256], P(None, 'dp', 'tensor')
- full_direction: bfloat16 [2, 8192, 256], P(None, 'dp', 'tensor')
The draws below stay inside these ranges and needn't reach their ends.
Inputs may be any that keep to these rules, and one draw needn't show every extreme that they name: Each row holds 1024 different frequencies, and 0 is one of them.
All inputs are finite; a program needn't handle non-finite values.
Results may differ from the reference program's by a relative error of at most 0.013.
Values may be sent and summed in bfloat16 or wider, within the bound.
A program may use at most 64 MiB of HBM per device.

```python
import math
import jax
import jax.numpy as jnp
from jax import lax

D = 8192
RANK = 1024
KV = 256
TOKENS = 2048
N_TENSOR = 2


def frequency_row(key, salt):
    chosen = jax.random.permutation(jax.random.fold_in(key, salt), D - 1)[:RANK] + 1
    position = jax.random.randint(jax.random.fold_in(key, salt + 100), (), 0, RANK)
    return chosen.at[position].set(0).astype(jnp.int32)


def draw_frequencies(key, part):
    return jnp.stack([frequency_row(key, 11), frequency_row(key, 12)]).astype(jnp.int32)


def set_ends(array, rng, smallest, high):
    shape = array.shape
    place = [jax.random.randint(jax.random.fold_in(rng, axis), (), 0, shape[axis]) for axis in range(len(shape))]
    array = array.at[tuple(place)].set(smallest)
    longest = shape.index(max(shape))
    place[longest] = (place[longest] + 1) % shape[longest]
    return array.at[tuple(place)].set(high)


def block_scale(key, dims, shards, least, top_value):
    def one(dim, shards_of):
        heights = jax.random.uniform(jax.random.fold_in(jax.random.fold_in(key, 6), dim), (shards_of,), jnp.float32, least / len(shards), top_value / len(shards))
        return jnp.repeat(jnp.exp(heights), dims[dim] // shards_of).reshape((-1,) + (1,) * (len(dims) - dim - 1))

    gain = one(*shards[0])
    for cut in shards[1:]:
        gain = gain * one(*cut)
    return gain


def centred(stream_key, shape, width, limit, split=(), kind=jnp.bfloat16):
    values = jax.random.normal(stream_key, shape, jnp.float32) * width
    if len(split) > 0:
        values = block_scale(stream_key, shape, split, -0.22, 0.18) * values
    return jnp.clip(values, min=-limit, max=limit).astype(kind)


def setup_inputs(seed: int = 0) -> dict:
    streams_of = jax.random.split(jax.random.key(seed), 8)
    return {
        "tokens": centred(streams_of[0], (TOKENS, D), 1.0, 6.0, ((0, 16), (1, 2))),
        "projection_weights": centred(streams_of[1], (2, D, KV), D ** -0.5, 0.0625, ((2, 2),)),
        "head_cotangent": centred(streams_of[2], (2, TOKENS, KV), 1.0, 6.0, ((1, 16), (2, 2))),
        "frequencies": draw_frequencies(jax.random.fold_in(streams_of[7], 71), 0),
        "sign_bits": set_ends((jax.random.randint(streams_of[4], (2, D), 0, 2) < 1).astype(jnp.int32), jax.random.fold_in(streams_of[4], 1), 0, 1),
        "first_moment": centred(streams_of[5], (2, RANK, KV), 1.0, 6.0, ((1, 16), (2, 2)), jnp.float32),
        "second_moment": jnp.clip(jnp.exp(math.log(2.0) - 2.3025851 * jax.random.uniform(streams_of[6], (2, RANK, KV), jnp.float32) ** block_scale(streams_of[6], (2, RANK, KV), ((1, 16), (2, 2)), -0.2, 0.2)), 0.2, 2.0),
    }


first_fix = 1.0 - 0.9 ** 10
second_fix = 1.0 - 0.95 ** 10
epsilon = 1e-08

def basis_rows(frequency, sign_part, offset, row_count, full_width):
    row_index = offset + lax.iota(jnp.int32, row_count)
    row_sign = lax.dynamic_slice_in_dim(sign_part, offset, row_count, 0)
    phase_index = (2 * row_index[:, None] + 1) * frequency[None, :] % (4 * full_width)
    angles = phase_index.astype(jnp.float32) * (math.pi / (2 * full_width))
    column_scale = jnp.where(frequency == 0, math.sqrt(1.0 / full_width), math.sqrt(2.0 / full_width)).astype(jnp.float32)
    signed = (2 * row_sign - 1).astype(jnp.float32)
    return (jnp.cos(angles) * column_scale[None, :] * signed[:, None]).astype(jnp.bfloat16)

def adam_update(gradient, first_moment, second_moment):
    new_first = 0.9 * first_moment + 0.1 * gradient
    new_second = 0.95 * second_moment + 0.05 * gradient * gradient
    direction = (new_first / first_fix / (jnp.sqrt(new_second / second_fix) + epsilon)).astype(jnp.bfloat16)
    return (new_first, new_second, direction)

def reference(tokens, projection_weights, head_cotangent, frequencies, sign_bits, first_moment, second_moment):
    token_count, full_width = tokens.shape
    head_width = projection_weights.shape[2] // N_TENSOR
    bases = [basis_rows(frequencies[matrix], sign_bits[matrix], 0, full_width, full_width) for matrix in range(2)]
    gradients = []
    for matrix in range(2):
        projected = jnp.dot(tokens, bases[matrix], preferred_element_type=jnp.float32).astype(jnp.bfloat16)
        low_rank = jnp.dot(projected.T, head_cotangent[matrix], preferred_element_type=jnp.float32)
        gradients.append(low_rank / math.sqrt(token_count))
    gradient = jnp.stack(gradients)
    new_first, new_second, direction = adam_update(gradient, first_moment, second_moment)
    full_direction = jnp.stack([jnp.dot(bases[matrix], direction[matrix], preferred_element_type=jnp.float32) for matrix in range(2)]).astype(jnp.bfloat16)
    summed = jnp.zeros((token_count, full_width), jnp.float32)
    for tensor_rank in range(N_TENSOR):
        columns = slice(tensor_rank * head_width, (tensor_rank + 1) * head_width)
        partial_sum = jnp.dot(head_cotangent[0][:, columns], projection_weights[0][:, columns].T, preferred_element_type=jnp.float32)
        partial_sum = partial_sum + jnp.dot(head_cotangent[1][:, columns], projection_weights[1][:, columns].T, preferred_element_type=jnp.float32)
        rounded = lax.optimization_barrier(partial_sum.astype(jnp.bfloat16))
        summed = summed + rounded.astype(jnp.float32)
    return (summed.astype(jnp.bfloat16), new_first, new_second, full_direction)
```

```python
import functools
import math

import jax
import jax.numpy as jnp
from jax import lax
from jax.experimental import pallas as pl
from jax.experimental.pallas import tpu as pltpu
from jax.sharding import PartitionSpec as P

first_fix = 1.0 - 0.9**10
second_fix = 1.0 - 0.95**10
epsilon = 1e-08
bf16, f32 = jnp.bfloat16, jnp.float32
PIECES = 4


def wrap(value, period):
    return value & (period - 1) if period & (period - 1) == 0 else lax.rem(value, period)


def trig(phase, width):
    phase = wrap(phase, 4 * width)
    shift = width.bit_length() - 1
    quarter = (phase + width // 2) >> shift if 1 << shift == width else lax.div(phase + width // 2, width)
    x = (phase - quarter * width).astype(f32) * (math.pi / (2 * width))
    y = x * x
    c = 1.0 + y * (-0.5 + y * (1 / 24 + y * (-1 / 720 + y * (1 / 40320 - y * (1 / 3628800)))))
    s = x * (1.0 + y * (-1 / 6 + y * (1 / 120 + y * (-1 / 5040 + y * (1 / 362880)))))
    quarter = quarter & 3
    odd = (quarter & 1) == 1
    cosine = jnp.where(odd, s, c) * jnp.where((quarter == 1) | (quarter == 2), -1.0, 1.0)
    sine = jnp.where(odd, c, s) * jnp.where(quarter >= 2, -1.0, 1.0)
    return cosine, sine


def dot_last(a, b):
    return lax.dot_general(a, b, (((1,), (1,)), ((), ())), preferred_element_type=f32)


def main_kernel(
    plan,
    tok_ref, w_ref, hc_ref, freq_ref, sign_ref, first_ref, second_ref,
    ig_ref, nf_ref, ns_ref, full_ref,
    tok_all, tok_s, freq, sgn, sgn_b, cb, sb, ca, sa, ra, rb, buf, back, sgn_col,
    hc_all, heads, pair_heads, quad_send, quad_recv, z_send, z_recv, mom, res, res_in, dirs, facc,
    f_send, f_recv, w_own, wp, g_acc, g_send, g_recv,
    loc, core_sems, hx_sems, hf_sems, wx_sems, wy_sems, quad_sems, z_sems, ag_sems,
):
    n_t, nz, nb, low_rows, token_count, width = plan
    rows, lw = tok_all.shape[1], tok_all.shape[2]
    rank = freq.shape[1]
    cr, cols = dirs.shape[1], dirs.shape[2]
    own = cr // 2
    zr = nb * cr
    own_rows = f_send.shape[0]
    half = lw // 2
    part = half // nb
    piece = part // PIECES
    wide = min(512, half)
    me_t, me_d = lax.axis_index("tensor"), lax.axis_index("dp")
    c, q = me_d % 2, me_d // 2
    y, z = q % nb, q // nb
    oc = 1 - c

    def dev(t, zz, yy, cc):
        return {"tensor": t, "dp": (zz * nb + yy) * 2 + cc}

    other = dev(me_t, z, y, oc)

    def xor(a, b):
        total, bit = 0, 1
        while bit < nz:
            total = total + bit * ((a // bit + b // bit) % 2)
            bit *= 2
        return total

    def remote(src, dst, send, recv, device):
        return pltpu.make_async_remote_copy(
            src_ref=src, dst_ref=dst, send_sem=send, recv_sem=recv,
            device_id=device, device_id_type=pl.DeviceIdType.MESH,
        )

    loads = [
        (freq_ref, freq),
        (tok_ref, tok_all.at[c]),
        (sign_ref.at[:, pl.ds(pl.multiple_of(me_t * lw, 128), lw)], sgn),
        (hc_ref, hc_all.at[me_t, c]),
        (sign_ref.at[:, pl.ds(pl.multiple_of(q * 2 * own_rows, 128), 2 * own_rows)], sgn_b),
        (first_ref.at[c], mom.at[0, c]),
        (second_ref.at[c], mom.at[1, c]),
        (w_ref.at[:, pl.ds(pl.multiple_of(me_t * lw + c * half, 128), half), :], w_own),
    ]
    loads = [pltpu.make_async_copy(a, b, loc.at[i]) for i, (a, b) in enumerate(loads)]
    for copy in loads:
        copy.start()

    barrier = pltpu.get_barrier_semaphore()
    peers = [other]
    for dt in range(n_t):
        for dy in range(nb):
            if dt or dy:
                peers.append(dev((me_t + dt) % n_t, z, (y + dy) % nb, c))
    for s in range(1, nz):
        peers.append(dev(me_t, xor(z, s), y, c))
    for device in peers:
        pl.semaphore_signal(barrier, inc=1, device_id=device, device_id_type=pl.DeviceIdType.MESH)

    loads[0].wait()
    f = jnp.where(c == 0, freq[0:1, :], freq[1:2, :])
    scale = jnp.where(f == 0, math.sqrt(1.0 / width), math.sqrt(2.0 / width)).astype(f32)

    def fill(cos_ref, sin_ref, start, stride, scaled):
        def block(r, carry):
            index = r * 8 + lax.broadcasted_iota(jnp.int32, (8, rank), 0)
            cosine, sine = trig((start + stride * index) * f, width)
            if scaled:
                cosine, sine = cosine * scale, sine * scale
            place = pl.ds(pl.multiple_of(r * 8, 8), 8)
            for k in range(nz):
                cos_ref[k, place, :] = cosine[:, k * zr : (k + 1) * zr]
                sin_ref[k, place, :] = sine[:, k * zr : (k + 1) * zr]
            return carry

        lax.fori_loop(0, cos_ref.shape[1] // 8, block, 0)

    fill(cb, sb, 1, 2, False)
    pl.semaphore_wait(barrier, len(peers))

    early = [
        remote(tok_ref, tok_all.at[c], core_sems.at[0, 0], core_sems.at[1, 0], other),
        remote(hc_ref, hc_all.at[me_t, c], core_sems.at[0, 1], core_sems.at[1, 1], other),
        remote(first_ref.at[oc], mom.at[0, c], core_sems.at[0, 2], core_sems.at[1, 2], other),
        remote(second_ref.at[oc], mom.at[1, c], core_sems.at[0, 3], core_sems.at[1, 3], other),
    ]

    def tensor_peer(s):
        return dev((me_t + s) % n_t, z, y, c)

    def hx_copy(s):
        return remote(hc_ref, hc_all.at[me_t, c], hx_sems.at[0, s - 1], hx_sems.at[1, s - 1], tensor_peer(s))

    def hf_copy(s):
        slot = hc_all.at[(me_t + n_t - s) % n_t, c]
        return remote(slot, slot, hf_sems.at[0, s - 1], hf_sems.at[1, s - 1], other)

    def wx_copy(s, p):
        row = y * part + p * piece
        at = pl.ds(pl.multiple_of(((me_t + s) % n_t) * lw + c * half + row, 16), piece)
        to = pl.ds(pl.multiple_of(row, 16), piece)
        return remote(
            w_ref.at[:, at, :], wp.at[s - 1, :, to, :],
            wx_sems.at[0, s - 1, p], wx_sems.at[1, s - 1, p], tensor_peer(s),
        )

    def wy_copy(s, p, dy):
        to = pl.ds(pl.multiple_of(y * part + p * piece, 16), piece)
        slot = wp.at[s - 1, :, to, :]
        return remote(
            slot, slot, wy_sems.at[0, s - 1, p, dy - 1], wy_sems.at[1, s - 1, p, dy - 1],
            dev(me_t, z, (y + dy) % nb, c),
        )

    early[0].start()
    for s in range(1, n_t):
        hx_copy(s).start()
    for copy in early[1:]:
        copy.start()
    for p in range(PIECES):
        for s in range(1, n_t):
            wx_copy(s, p).start()

    fill(ca, sa, 2 * me_t * lw, 2 * low_rows, True)
    fill(ra, rb, 2 * q * 2 * own_rows, 2 * low_rows, True)

    def sign_tokens(k):
        step = min(512, lw)

        def tile(j, carry):
            place = pl.ds(pl.multiple_of(j * step, step), step)
            row = jnp.where(c == 0, sgn[0:1, place], sgn[1:2, place])
            row = (2 * row - 1).astype(f32).astype(bf16)
            tok_s[pl.ds(k, 1), :, place] = tok_all[pl.ds(k, 1), :, place] * row
            return carry

        lax.fori_loop(0, lw // step, tile, 0)

    loads[1].wait()
    loads[2].wait()
    sign_tokens(c)
    for s in range(1, n_t):
        hx_copy(s).wait_recv()
        hf_copy(s).start()
    early[0].wait_recv()
    sign_tokens(oc)

    def tables(a_ref, b_ref, h, k):
        row = pl.ds(h, 1)
        return (a_ref[k, row, :] * cb[k] - b_ref[k, row, :] * sb[k]).astype(bf16)

    def quad_copy(i, dt, dy):
        slot = dt * nb + dy - 1
        t, yy = (me_t + dt) % n_t, (y + dy) % nb
        return remote(
            quad_send.at[i, t, yy], quad_recv.at[i, slot],
            quad_sems.at[0, i, slot], quad_sems.at[1, i, slot], dev(t, z, yy, c),
        )

    quad_slots = [(dt, dy) for dt in range(n_t) for dy in range(nb) if dt or dy]

    def z_copy(i):
        return remote(
            z_send.at[i], z_recv.at[i], z_sems.at[0, i], z_sems.at[1, i], dev(me_t, xor(z, nz - 1 - i), y, c)
        )

    def reduced(i):
        total = quad_send[i, me_t, y].astype(f32)
        for dt, dy in quad_slots:
            quad_copy(i, dt, dy).wait_recv()
            total = total + quad_recv[i, dt * nb + dy - 1].astype(f32)
        return total

    def pass_on(i):
        z_send[i] = reduced(i).astype(bf16)
        z_copy(i).start()

    def chunk(i, carry):
        k = xor(z, nz - 1 - i)

        def build(h, carry):
            buf[pl.ds(pl.multiple_of(h * low_rows, low_rows), low_rows), :] = tables(ca, sa, h, k)
            return carry

        lax.fori_loop(0, lw // low_rows, build, 0, unroll=2)
        projected = jnp.dot(tok_s[...].reshape(2 * rows, lw), buf[...], preferred_element_type=f32).astype(bf16)

        @pl.when(i == 0)
        def _():
            loads[3].wait()
            early[1].wait_recv()
            for s in range(1, n_t):
                hf_copy(s).wait_recv()
            for t in range(n_t):
                heads[:, t * cols : (t + 1) * cols] = hc_all[t, :, pl.ds(c, 1)].reshape(2 * rows, cols)
                for m in range(2):
                    pair_heads[t, :, m * cols : (m + 1) * cols] = hc_all[t, :, m].reshape(2 * rows, cols)

        low = lax.dot_general(
            projected, heads[...], (((0,), (0,)), ((), ())), preferred_element_type=f32
        ).astype(bf16)
        for t in range(n_t):
            for yy in range(nb):
                quad_send[i, t, yy] = low[yy * cr : (yy + 1) * cr, t * cols : (t + 1) * cols]
        for dt, dy in quad_slots:
            quad_copy(i, dt, dy).start()

        @pl.when(i > 0)
        def _():
            pass_on(i - 1)

        return carry

    lax.fori_loop(0, nz, chunk, 0)

    def back_rows(h, carry):
        place = pl.ds(pl.multiple_of(h * low_rows, low_rows), low_rows)
        for k in range(nz):
            back[k, place, :] = tables(ra, rb, h, k)
        return carry

    lax.fori_loop(0, back.shape[1] // low_rows, back_rows, 0)
    loads[4].wait()
    lane = min(128, 2 * own_rows)
    for b in range(2 * own_rows // lane):
        at = slice(b * lane, (b + 1) * lane)
        row = (2 * jnp.where(c == 0, sgn_b[0:1, at], sgn_b[1:2, at]) - 1).astype(f32)
        sgn_col[b * lane : (b + 1) * lane, :] = jnp.broadcast_to(row, (128, lane)).T
    loads[7].wait()

    def own_gradient(j, carry):
        place = pl.ds(pl.multiple_of(j * wide, wide), wide)
        w = jnp.concatenate([w_own[m, place, :] for m in range(2)], axis=1)
        g_acc[:, place] = dot_last(pair_heads[me_t], w)
        return carry

    lax.fori_loop(0, half // wide, own_gradient, 0)
    for i in (5, 6):
        loads[i].wait()
    for i in (2, 3):
        early[i].wait_recv()

    total = reduced(nz - 1)
    for i in range(nz - 1):
        z_copy(i).wait_recv()
        total = total + z_recv[i].astype(f32)
    gradient = (total / math.sqrt(token_count)).reshape(2, own, cols)
    new_first = 0.9 * mom[0] + 0.1 * gradient
    new_second = 0.95 * mom[1] + 0.05 * gradient * gradient
    direction = new_first / first_fix / (jnp.sqrt(new_second / second_fix) + epsilon)
    dirs[pl.ds(z * nb + y, 1)] = direction.astype(bf16).reshape(1, cr, cols)

    def ag_copy(s, dy):
        if dy == 0:
            slot = dirs.at[z * nb + y]
            return remote(slot, slot, ag_sems.at[0, s, 0], ag_sems.at[1, s, 0], dev(me_t, xor(z, s), y, c))
        slot = dirs.at[xor(z, s) * nb + y]
        return remote(
            slot, slot, ag_sems.at[0, s, dy], ag_sems.at[1, s, dy], dev(me_t, z, (y + dy) % nb, c)
        )

    for s in range(nz - 1, 0, -1):
        ag_copy(s, 0).start()
    for dy in range(1, nb):
        ag_copy(0, dy).start()
    res[0] = new_first
    res[1] = new_second
    res_copies = [
        remote(res.at[k, oc], res_in.at[k], core_sems.at[0, 4 + k], core_sems.at[1, 4 + k], other)
        for k in range(2)
    ]
    for copy in res_copies:
        copy.start()

    def relay(p):
        for s in range(1, n_t):
            wx_copy(s, p).wait_recv()
            for dy in range(1, nb):
                wy_copy(s, p, dy).start()

    for p in range(PIECES):
        relay(p)
    for s in range(1, nz):
        ag_copy(s, 0).wait_recv()
        for dy in range(1, nb):
            ag_copy(s, dy).start()
    facc[...] = jnp.zeros_like(facc)
    for s in range(nz):
        for dy in range(1, nb):
            ag_copy(s, dy).wait_recv()
        zz = xor(z, s)
        block = dirs[pl.ds(zz * nb, nb)].reshape(zr, cols)
        facc[...] += jnp.dot(back[zz], block, preferred_element_type=f32)

    def finished(k):
        place = pl.ds(pl.multiple_of(k * own_rows, own_rows), own_rows)
        value, signs = facc[place, :], sgn_col[place, :]
        return jnp.concatenate(
            [value[:, j : j + 128] * signs for j in range(0, cols, 128)], axis=1
        ).astype(bf16)

    f_send[...] = finished(oc)
    f_copy = remote(f_send, f_recv, core_sems.at[0, 6], core_sems.at[1, 6], other)
    f_copy.start()
    full_ref[pl.ds(c, 1)] = finished(c)[None]

    for p in range(PIECES):
        for s in range(1, n_t):
            for dy in range(1, nb):
                wy_copy(s, p, dy).wait_recv()

    def add_gradient(j, carry):
        place = pl.ds(pl.multiple_of(j * wide, wide), wide)
        value = g_acc[:, place]
        for s in range(1, n_t):
            w = jnp.concatenate([wp[s - 1, m, place, :] for m in range(2)], axis=1)
            value = value + dot_last(pair_heads[(me_t + n_t - s) % n_t], w)
        g_acc[:, place] = value
        g_send[:, place] = g_acc[pl.ds(pl.multiple_of(oc * rows, rows), rows), place].astype(bf16)
        mine = g_acc[pl.ds(pl.multiple_of(c * rows, rows), rows), place].astype(bf16)
        ig_ref[pl.ds(c, 1), :, place] = mine[None]
        return carry

    lax.fori_loop(0, half // wide, add_gradient, 0)
    g_copy = remote(g_send, g_recv, core_sems.at[0, 7], core_sems.at[1, 7], other)
    g_copy.start()

    nf_ref[pl.ds(c, 1)] = res[0, pl.ds(c, 1)]
    ns_ref[pl.ds(c, 1)] = res[1, pl.ds(c, 1)]
    for copy in res_copies:
        copy.wait_recv()
    nf_ref[pl.ds(oc, 1)] = res_in[0][None]
    ns_ref[pl.ds(oc, 1)] = res_in[1][None]
    f_copy.wait_recv()
    full_ref[pl.ds(oc, 1)] = f_recv[...][None]
    g_copy.wait_recv()
    ig_ref[pl.ds(oc, 1)] = g_recv[...][None]

    for copy in early + res_copies + [f_copy, g_copy]:
        copy.wait_send()
    for s in range(1, n_t):
        hx_copy(s).wait_send()
        hf_copy(s).wait_send()
        for p in range(PIECES):
            wx_copy(s, p).wait_send()
            for dy in range(1, nb):
                wy_copy(s, p, dy).wait_send()

    def sent(i, carry):
        for dt, dy in quad_slots:
            quad_copy(i, dt, dy).wait_send()
        return carry

    lax.fori_loop(0, nz, sent, 0)
    for i in range(nz - 1):
        z_copy(i).wait_send()
    for s in range(nz):
        for dy in range(nb):
            if s or dy:
                ag_copy(s, dy).wait_send()


def write_kernel(ig, nf, ns, full, ig_out, nf_out, ns_out, full_out, sems):
    half = ig.shape[2]
    copies = [(ig.at[k], ig_out.at[:, k * half : (k + 1) * half]) for k in range(2)]
    copies += [(full, full_out), (nf, nf_out), (ns, ns_out)]
    copies = [pltpu.make_async_copy(a, b, sems.at[i]) for i, (a, b) in enumerate(copies)]
    for copy in copies:
        copy.start()
    for copy in copies:
        copy.wait()


def shards(
    tokens, projection_weights, head_cotangent, frequencies, sign_bits, first_moment, second_moment
):
    rows, lw = tokens.shape
    n_t, n_dp = lax.axis_size("tensor"), lax.axis_size("dp")
    width = lw * n_t
    rank = frequencies.shape[1]
    own, cols = first_moment.shape[1], first_moment.shape[2]
    own_rows = projection_weights.shape[1] // n_dp
    chips = n_dp // 2
    cr = 2 * own
    nb = 2
    while nb * cr % 128:
        nb *= 2
    nz = chips // nb
    zr = nb * cr
    low_rows = min(128, 2 * own_rows)
    up8 = lambda n: -(-n // 8) * 8
    half = lw // 2
    group = n_t * nb - 1

    anywhere, vmem = pl.BlockSpec(memory_space=pltpu.HBM), pl.BlockSpec(memory_space=pltpu.VMEM)
    dma = pltpu.SemaphoreType.DMA
    V = pltpu.VMEM
    plan = (n_t, nz, nb, low_rows, rows * n_dp, width)
    ig, nf, ns, full = pl.pallas_call(
        functools.partial(main_kernel, plan),
        out_shape=(
            jax.ShapeDtypeStruct((2, rows, half), bf16),
            jax.ShapeDtypeStruct((2, own, cols), f32),
            jax.ShapeDtypeStruct((2, own, cols), f32),
            jax.ShapeDtypeStruct((2, own_rows, cols), bf16),
        ),
        in_specs=[anywhere] * 7,
        out_specs=(vmem,) * 4,
        scratch_shapes=[
            V((2, rows, lw), bf16), V((2, rows, lw), bf16), V((2, rank), jnp.int32),
            V((2, lw), jnp.int32), V((2, 2 * own_rows), jnp.int32),
            V((nz, low_rows, zr), f32), V((nz, low_rows, zr), f32),
            V((nz, up8(lw // low_rows), zr), f32), V((nz, up8(lw // low_rows), zr), f32),
            V((nz, up8(2 * own_rows // low_rows), zr), f32), V((nz, up8(2 * own_rows // low_rows), zr), f32),
            V((lw, zr), bf16), V((nz, 2 * own_rows, zr), bf16), V((2 * own_rows, 128), f32),
            V((n_t, 2, 2, rows, cols), bf16), V((2 * rows, n_t * cols), bf16), V((n_t, 2 * rows, 2 * cols), bf16),
            V((nz, n_t, nb, cr, cols), bf16), V((nz, group, cr, cols), bf16),
            V((nz, cr, cols), bf16), V((nz, cr, cols), bf16),
            V((2, 2, own, cols), f32), V((2, 2, own, cols), f32), V((2, own, cols), f32),
            V((nz * nb, cr, cols), bf16), V((2 * own_rows, cols), f32),
            V((own_rows, cols), bf16), V((own_rows, cols), bf16),
            V((2, half, cols), bf16), V((n_t - 1, 2, half, cols), bf16),
            V((2 * rows, half), f32), V((rows, half), bf16), V((rows, half), bf16),
            dma((8,)), dma((2, 8)), dma((2, n_t - 1)), dma((2, n_t - 1)),
            dma((2, n_t - 1, PIECES)), dma((2, n_t - 1, PIECES, nb - 1)),
            dma((2, nz, group)), dma((2, nz)), dma((2, nz, nb)),
        ],
        compiler_params=pltpu.CompilerParams(
            collective_id=0, has_side_effects=True, vmem_limit_bytes=48 * 1024 * 1024
        ),
    )(tokens, projection_weights, head_cotangent, frequencies, sign_bits, first_moment, second_moment)
    return pl.pallas_call(
        write_kernel,
        out_shape=(
            jax.ShapeDtypeStruct((rows, lw), bf16),
            jax.ShapeDtypeStruct((2, own, cols), f32),
            jax.ShapeDtypeStruct((2, own, cols), f32),
            jax.ShapeDtypeStruct((2, own_rows, cols), bf16),
        ),
        in_specs=[vmem] * 4,
        out_specs=(anywhere,) * 4,
        scratch_shapes=[dma((5,))],
        compiler_params=pltpu.CompilerParams(vmem_limit_bytes=8 * 1024 * 1024),
    )(ig, nf, ns, full)


def solution(mesh):
    in_specs = (
        P("dp", "tensor"),
        P(None, None, "tensor"),
        P(None, "dp", "tensor"),
        P(),
        P(),
        P(None, "dp", "tensor"),
        P(None, "dp", "tensor"),
    )
    out_specs = (
        P("dp", "tensor"),
        P(None, "dp", "tensor"),
        P(None, "dp", "tensor"),
        P(None, "dp", "tensor"),
    )
    return jax.shard_map(shards, mesh=mesh, in_specs=in_specs, out_specs=out_specs, check_vma=False)
```

```python
import functools
import math

import jax
import jax.numpy as jnp
from jax import lax
from jax.experimental import pallas as pl
from jax.experimental.pallas import tpu as pltpu
from jax.sharding import PartitionSpec as P

first_fix = 1.0 - 0.9**10
second_fix = 1.0 - 0.95**10
epsilon = 1e-08
bf16, f32 = jnp.bfloat16, jnp.float32
RELAY0 = 2


def wrap(value, period):
    return value & (period - 1) if period & (period - 1) == 0 else lax.rem(value, period)


def trig(phase, width):
    phase = wrap(phase, 4 * width)
    shift = width.bit_length() - 1
    quarter = (phase + width // 2) >> shift if 1 << shift == width else lax.div(phase + width // 2, width)
    x = (phase - quarter * width).astype(f32) * (math.pi / (2 * width))
    y = x * x
    c = 1.0 + y * (-0.5 + y * (1 / 24 + y * (-1 / 720 + y * (1 / 40320 - y * (1 / 3628800)))))
    s = x * (1.0 + y * (-1 / 6 + y * (1 / 120 + y * (-1 / 5040 + y * (1 / 362880)))))
    quarter = quarter & 3
    odd = (quarter & 1) == 1
    cosine = jnp.where(odd, s, c) * jnp.where((quarter == 1) | (quarter == 2), -1.0, 1.0)
    sine = jnp.where(odd, c, s) * jnp.where(quarter >= 2, -1.0, 1.0)
    return cosine, sine


def dot_last(a, b):
    return lax.dot_general(a, b, (((1,), (1,)), ((), ())), preferred_element_type=f32)


def main_kernel(
    plan,
    tok_ref, w_ref, hc_ref, freq_ref, sign_ref, first_ref, second_ref,
    ig_ref, nf_ref, ns_ref, full_ref,
    tok_all, tok_s, freq, sgn, sgn_b, cb, sb, ca, sa, ra, rb, buf, back, sgn_col,
    hc_all, heads, pair_heads, quad_send, quad_recv, z_send, z_recv, mom, res, res_in, dirs, facc,
    f_send, f_recv, w_own, wp, g_acc, g_send, g_recv,
    loc, core_sems, hx_sems, hf_sems, wx_sems, wy_sems, wz_sems, quad_sems, z_sems, ag_sems,
):
    n_t, nz, nb, low_rows, token_count, width = plan
    rows, lw = tok_all.shape[1], tok_all.shape[2]
    rank = freq.shape[1]
    cr, cols = dirs.shape[1], dirs.shape[2]
    own = cr // 2
    zr = nb * cr
    own_rows = f_send.shape[0]
    half = lw // 2
    part = half // (2 * nb)
    piece = part // 2
    wide = min(512, half)
    me_t, me_d = lax.axis_index("tensor"), lax.axis_index("dp")
    c, q = me_d % 2, me_d // 2
    y, z = q % nb, q // nb
    oc = 1 - c

    def dev(t, zz, yy, cc):
        return {"tensor": t, "dp": (zz * nb + yy) * 2 + cc}

    other = dev(me_t, z, y, oc)

    def xor(a, b):
        total, bit = 0, 1
        while bit < nz:
            total = total + bit * ((a // bit + b // bit) % 2)
            bit *= 2
        return total

    def remote(src, dst, send, recv, device):
        return pltpu.make_async_remote_copy(
            src_ref=src, dst_ref=dst, send_sem=send, recv_sem=recv,
            device_id=device, device_id_type=pl.DeviceIdType.MESH,
        )

    loads = [
        (freq_ref, freq),
        (tok_ref, tok_all.at[c]),
        (sign_ref.at[:, pl.ds(pl.multiple_of(me_t * lw, 128), lw)], sgn),
        (hc_ref, hc_all.at[me_t, c]),
        (sign_ref.at[:, pl.ds(pl.multiple_of(q * 2 * own_rows, 128), 2 * own_rows)], sgn_b),
        (first_ref.at[c], mom.at[0, c]),
        (second_ref.at[c], mom.at[1, c]),
        (w_ref.at[:, pl.ds(pl.multiple_of(me_t * lw + c * half, 128), half), :], w_own),
    ]
    loads = [pltpu.make_async_copy(a, b, loc.at[i]) for i, (a, b) in enumerate(loads)]
    for copy in loads:
        copy.start()

    barrier = pltpu.get_barrier_semaphore()
    peers = [other]
    for dt in range(n_t):
        for dy in range(nb):
            if dt or dy:
                peers.append(dev((me_t + dt) % n_t, z, (y + dy) % nb, c))
    for s in range(1, nz):
        peers.append(dev(me_t, xor(z, s), y, c))
    for device in peers:
        pl.semaphore_signal(barrier, inc=1, device_id=device, device_id_type=pl.DeviceIdType.MESH)

    pl.semaphore_wait(barrier, len(peers))

    early = [
        remote(tok_ref, tok_all.at[c], core_sems.at[0, 0], core_sems.at[1, 0], other),
        remote(hc_ref, hc_all.at[me_t, c], core_sems.at[0, 1], core_sems.at[1, 1], other),
        remote(first_ref.at[oc], mom.at[0, c], core_sems.at[0, 2], core_sems.at[1, 2], other),
        remote(second_ref.at[oc], mom.at[1, c], core_sems.at[0, 3], core_sems.at[1, 3], other),
    ]

    def tensor_peer(s):
        return dev((me_t + s) % n_t, z, y, c)

    def hx_copy(s):
        return remote(hc_ref, hc_all.at[me_t, c], hx_sems.at[0, s - 1], hx_sems.at[1, s - 1], tensor_peer(s))

    def hf_copy(s):
        slot = hc_all.at[(me_t + n_t - s) % n_t, c]
        return remote(slot, slot, hf_sems.at[0, s - 1], hf_sems.at[1, s - 1], other)

    def rows_of(yy, zl, p):
        return pl.multiple_of((yy * 2 + zl) * part + p * piece, 16)

    zl = z % 2

    def wx_copy(s, k):
        yy, zz, p = (y, zl, k) if k < 2 else ((y + k - 1) % nb, 1 - zl, 1)
        row = rows_of(yy, zz, p)
        at = pl.ds(pl.multiple_of(((me_t + s) % n_t) * lw + c * half + row, 16), piece)
        return remote(
            w_ref.at[:, at, :], wp.at[s - 1, :, pl.ds(row, piece), :],
            wx_sems.at[0, s - 1, k], wx_sems.at[1, s - 1, k], tensor_peer(s),
        )

    def wy_copy(s, p, dy):
        slot = wp.at[s - 1, :, pl.ds(rows_of(y, zl, p), piece), :]
        return remote(
            slot, slot, wy_sems.at[0, s - 1, p, dy - 1], wy_sems.at[1, s - 1, p, dy - 1],
            dev(me_t, z, (y + dy) % nb, c),
        )

    def wz_copy(s, k):
        yy, p = (y, k) if k < 2 else ((y + nb - (k - 1)) % nb, 0)
        slot = wp.at[s - 1, :, pl.ds(rows_of(yy, zl, p), piece), :]
        return remote(
            slot, slot, wz_sems.at[0, s - 1, k], wz_sems.at[1, s - 1, k], dev(me_t, xor(z, 1), y, c)
        )

    tensor_peers, y_peers = range(1, n_t), range(1, nb)

    def fetch(k):
        for s in tensor_peers:
            wx_copy(s, k).start()

    def relay(p):
        for s in tensor_peers:
            wx_copy(s, p).wait_recv()
            for dy in y_peers:
                wy_copy(s, p, dy).start()
            wz_copy(s, p).start()

    def forward():
        for s in tensor_peers:
            for dy in y_peers:
                wy_copy(s, 0, dy).wait_recv()
                wz_copy(s, 1 + dy).start()

    early[0].start()
    for s in range(1, n_t):
        hx_copy(s).start()
    for copy in early[1:]:
        copy.start()
    fetch(0)
    fetch(1)

    loads[0].wait()
    f = jnp.where(c == 0, freq[0:1, :], freq[1:2, :])
    scale = jnp.where(f == 0, math.sqrt(1.0 / width), math.sqrt(2.0 / width)).astype(f32)

    def fill(cos_ref, sin_ref, start, stride, scaled):
        def block(r, carry):
            index = r * 8 + lax.broadcasted_iota(jnp.int32, (8, rank), 0)
            cosine, sine = trig((start + stride * index) * f, width)
            if scaled:
                cosine, sine = cosine * scale, sine * scale
            place = pl.ds(pl.multiple_of(r * 8, 8), 8)
            for k in range(nz):
                cos_ref[k, place, :] = cosine[:, k * zr : (k + 1) * zr]
                sin_ref[k, place, :] = sine[:, k * zr : (k + 1) * zr]
            return carry

        lax.fori_loop(0, cos_ref.shape[1] // 8, block, 0)

    fill(cb, sb, 1, 2, False)
    fill(ca, sa, 2 * me_t * lw, 2 * low_rows, True)
    fill(ra, rb, 2 * q * 2 * own_rows, 2 * low_rows, True)

    def sign_tokens(k):
        step = min(512, lw)

        def tile(j, carry):
            place = pl.ds(pl.multiple_of(j * step, step), step)
            row = jnp.where(c == 0, sgn[0:1, place], sgn[1:2, place])
            row = (2 * row - 1).astype(f32).astype(bf16)
            tok_s[pl.ds(k, 1), :, place] = tok_all[pl.ds(k, 1), :, place] * row
            return carry

        lax.fori_loop(0, lw // step, tile, 0)

    loads[1].wait()
    loads[2].wait()
    sign_tokens(c)
    for s in range(1, n_t):
        hx_copy(s).wait_recv()
        hf_copy(s).start()
    early[0].wait_recv()
    sign_tokens(oc)

    def tables(a_ref, b_ref, h, k):
        row = pl.ds(h, 1)
        return (a_ref[k, row, :] * cb[k] - b_ref[k, row, :] * sb[k]).astype(bf16)

    def quad_copy(i, dt, dy):
        slot = dt * nb + dy - 1
        t, yy = (me_t + dt) % n_t, (y + dy) % nb
        return remote(
            quad_send.at[i, t, yy], quad_recv.at[i, slot],
            quad_sems.at[0, i, slot], quad_sems.at[1, i, slot], dev(t, z, yy, c),
        )

    quad_slots = [(dt, dy) for dt in range(n_t) for dy in range(nb) if dt or dy]

    def z_copy(i):
        return remote(
            z_send.at[i], z_recv.at[i], z_sems.at[0, i], z_sems.at[1, i], dev(me_t, xor(z, nz - 1 - i), y, c)
        )

    def reduced(i):
        total = quad_send[i, me_t, y].astype(f32)
        for dt, dy in quad_slots:
            quad_copy(i, dt, dy).wait_recv()
            total = total + quad_recv[i, dt * nb + dy - 1].astype(f32)
        return total

    def pass_on(i):
        z_send[i] = reduced(i).astype(bf16)
        z_copy(i).start()

    def chunk(i, carry):
        k = xor(z, nz - 1 - i)

        def build(h, carry):
            buf[pl.ds(pl.multiple_of(h * low_rows, low_rows), low_rows), :] = tables(ca, sa, h, k)
            return carry

        lax.fori_loop(0, lw // low_rows, build, 0, unroll=2)
        projected = jnp.dot(tok_s[...].reshape(2 * rows, lw), buf[...], preferred_element_type=f32).astype(bf16)

        @pl.when(i == 0)
        def _():
            loads[3].wait()
            early[1].wait_recv()
            for s in range(1, n_t):
                hf_copy(s).wait_recv()
            for t in range(n_t):
                heads[:, t * cols : (t + 1) * cols] = hc_all[t, :, pl.ds(c, 1)].reshape(2 * rows, cols)
                for m in range(2):
                    pair_heads[t, :, m * cols : (m + 1) * cols] = hc_all[t, :, m].reshape(2 * rows, cols)

        low = lax.dot_general(
            projected, heads[...], (((0,), (0,)), ((), ())), preferred_element_type=f32
        ).astype(bf16)
        for t in range(n_t):
            for yy in range(nb):
                quad_send[i, t, yy] = low[yy * cr : (yy + 1) * cr, t * cols : (t + 1) * cols]
        for dt, dy in quad_slots:
            quad_copy(i, dt, dy).start()

        @pl.when(i > 0)
        def _():
            pass_on(i - 1)

        @pl.when(i == RELAY0)
        def _():
            relay(0)

        return carry

    lax.fori_loop(0, nz, chunk, 0)

    for k in range(2, nb + 1):
        fetch(k)
    def back_rows(h, carry):
        place = pl.ds(pl.multiple_of(h * low_rows, low_rows), low_rows)
        for k in range(nz):
            back[k, place, :] = tables(ra, rb, h, k)
        return carry

    lax.fori_loop(0, back.shape[1] // low_rows, back_rows, 0)
    loads[4].wait()
    lane = min(128, 2 * own_rows)
    for b in range(2 * own_rows // lane):
        at = slice(b * lane, (b + 1) * lane)
        row = (2 * jnp.where(c == 0, sgn_b[0:1, at], sgn_b[1:2, at]) - 1).astype(f32)
        sgn_col[b * lane : (b + 1) * lane, :] = jnp.broadcast_to(row, (128, lane)).T
    loads[7].wait()

    def own_gradient(j, carry):
        place = pl.ds(pl.multiple_of(j * wide, wide), wide)
        w = jnp.concatenate([w_own[m, place, :] for m in range(2)], axis=1)
        g_acc[:, place] = dot_last(pair_heads[me_t], w)
        return carry

    lax.fori_loop(0, half // wide, own_gradient, 0)
    relay(1)
    for i in (5, 6):
        loads[i].wait()
    for i in (2, 3):
        early[i].wait_recv()

    total = reduced(nz - 1)
    for i in range(nz - 1):
        z_copy(i).wait_recv()
        total = total + z_recv[i].astype(f32)
    gradient = (total / math.sqrt(token_count)).reshape(2, own, cols)
    new_first = 0.9 * mom[0] + 0.1 * gradient
    new_second = 0.95 * mom[1] + 0.05 * gradient * gradient
    direction = new_first / first_fix / (jnp.sqrt(new_second / second_fix) + epsilon)
    dirs[pl.ds(z * nb + y, 1)] = direction.astype(bf16).reshape(1, cr, cols)

    def ag_copy(s, dy):
        if dy == 0:
            slot = dirs.at[z * nb + y]
            return remote(slot, slot, ag_sems.at[0, s, 0], ag_sems.at[1, s, 0], dev(me_t, xor(z, s), y, c))
        slot = dirs.at[xor(z, s) * nb + y]
        return remote(
            slot, slot, ag_sems.at[0, s, dy], ag_sems.at[1, s, dy], dev(me_t, z, (y + dy) % nb, c)
        )

    for s in range(nz - 1, 0, -1):
        ag_copy(s, 0).start()
    for dy in range(1, nb):
        ag_copy(0, dy).start()
    res[0] = new_first
    res[1] = new_second
    res_copies = [
        remote(res.at[k, oc], res_in.at[k], core_sems.at[0, 4 + k], core_sems.at[1, 4 + k], other)
        for k in range(2)
    ]
    for copy in res_copies:
        copy.start()

    forward()
    for s in range(1, nz):
        ag_copy(s, 0).wait_recv()
        for dy in range(1, nb):
            ag_copy(s, dy).start()
    facc[...] = jnp.zeros_like(facc)
    for s in range(nz):
        for dy in range(1, nb):
            ag_copy(s, dy).wait_recv()
        zz = xor(z, s)
        block = dirs[pl.ds(zz * nb, nb)].reshape(zr, cols)
        facc[...] += jnp.dot(back[zz], block, preferred_element_type=f32)

    def finished(k):
        place = pl.ds(pl.multiple_of(k * own_rows, own_rows), own_rows)
        value, signs = facc[place, :], sgn_col[place, :]
        return jnp.concatenate(
            [value[:, j : j + 128] * signs for j in range(0, cols, 128)], axis=1
        ).astype(bf16)

    f_send[...] = finished(oc)
    f_copy = remote(f_send, f_recv, core_sems.at[0, 6], core_sems.at[1, 6], other)
    f_copy.start()
    full_ref[pl.ds(c, 1)] = finished(c)[None]

    for s in tensor_peers:
        for dy in y_peers:
            wy_copy(s, 1, dy).wait_recv()
            wx_copy(s, 1 + dy).wait_recv()
        for k in range(nb + 1):
            wz_copy(s, k).wait_recv()

    def add_gradient(j, carry):
        place = pl.ds(pl.multiple_of(j * wide, wide), wide)
        value = g_acc[:, place]
        for s in range(1, n_t):
            w = jnp.concatenate([wp[s - 1, m, place, :] for m in range(2)], axis=1)
            value = value + dot_last(pair_heads[(me_t + n_t - s) % n_t], w)
        g_acc[:, place] = value
        g_send[:, place] = g_acc[pl.ds(pl.multiple_of(oc * rows, rows), rows), place].astype(bf16)
        mine = g_acc[pl.ds(pl.multiple_of(c * rows, rows), rows), place].astype(bf16)
        ig_ref[pl.ds(c, 1), :, place] = mine[None]
        return carry

    lax.fori_loop(0, half // wide, add_gradient, 0)
    g_copy = remote(g_send, g_recv, core_sems.at[0, 7], core_sems.at[1, 7], other)
    g_copy.start()

    nf_ref[pl.ds(c, 1)] = res[0, pl.ds(c, 1)]
    ns_ref[pl.ds(c, 1)] = res[1, pl.ds(c, 1)]
    for copy in res_copies:
        copy.wait_recv()
    nf_ref[pl.ds(oc, 1)] = res_in[0][None]
    ns_ref[pl.ds(oc, 1)] = res_in[1][None]
    f_copy.wait_recv()
    full_ref[pl.ds(oc, 1)] = f_recv[...][None]
    g_copy.wait_recv()
    ig_ref[pl.ds(oc, 1)] = g_recv[...][None]

    for copy in early + res_copies + [f_copy, g_copy]:
        copy.wait_send()
    for s in range(1, n_t):
        hx_copy(s).wait_send()
        hf_copy(s).wait_send()
        for k in range(nb + 1):
            wx_copy(s, k).wait_send()
            wz_copy(s, k).wait_send()
        for dy in y_peers:
            for p in range(2):
                wy_copy(s, p, dy).wait_send()

    def sent(i, carry):
        for dt, dy in quad_slots:
            quad_copy(i, dt, dy).wait_send()
        return carry

    lax.fori_loop(0, nz, sent, 0)
    for i in range(nz - 1):
        z_copy(i).wait_send()
    for s in range(nz):
        for dy in range(nb):
            if s or dy:
                ag_copy(s, dy).wait_send()


def write_kernel(ig, nf, ns, full, ig_out, nf_out, ns_out, full_out, sems):
    half = ig.shape[2]
    copies = [(ig.at[k], ig_out.at[:, k * half : (k + 1) * half]) for k in range(2)]
    copies += [(full, full_out), (nf, nf_out), (ns, ns_out)]
    copies = [pltpu.make_async_copy(a, b, sems.at[i]) for i, (a, b) in enumerate(copies)]
    for copy in copies:
        copy.start()
    for copy in copies:
        copy.wait()


def shards(
    tokens, projection_weights, head_cotangent, frequencies, sign_bits, first_moment, second_moment
):
    rows, lw = tokens.shape
    n_t, n_dp = lax.axis_size("tensor"), lax.axis_size("dp")
    width = lw * n_t
    rank = frequencies.shape[1]
    own, cols = first_moment.shape[1], first_moment.shape[2]
    own_rows = projection_weights.shape[1] // n_dp
    chips = n_dp // 2
    cr = 2 * own
    nb = 2
    while nb * cr % 128:
        nb *= 2
    nz = chips // nb
    zr = nb * cr
    low_rows = min(128, 2 * own_rows)
    up8 = lambda n: -(-n // 8) * 8
    half = lw // 2
    group = n_t * nb - 1

    anywhere, vmem = pl.BlockSpec(memory_space=pltpu.HBM), pl.BlockSpec(memory_space=pltpu.VMEM)
    dma = pltpu.SemaphoreType.DMA
    V = pltpu.VMEM
    args = (tokens, projection_weights, head_cotangent, frequencies, sign_bits, first_moment, second_moment)
    plan = (n_t, nz, nb, low_rows, rows * n_dp, width)
    ig, nf, ns, full = pl.pallas_call(
        functools.partial(main_kernel, plan),
        out_shape=(
            jax.ShapeDtypeStruct((2, rows, half), bf16),
            jax.ShapeDtypeStruct((2, own, cols), f32),
            jax.ShapeDtypeStruct((2, own, cols), f32),
            jax.ShapeDtypeStruct((2, own_rows, cols), bf16),
        ),
        in_specs=[anywhere] * 7,
        out_specs=(vmem,) * 4,
        scratch_shapes=[
            V((2, rows, lw), bf16), V((2, rows, lw), bf16), V((2, rank), jnp.int32),
            V((2, lw), jnp.int32), V((2, 2 * own_rows), jnp.int32),
            V((nz, low_rows, zr), f32), V((nz, low_rows, zr), f32),
            V((nz, up8(lw // low_rows), zr), f32), V((nz, up8(lw // low_rows), zr), f32),
            V((nz, up8(2 * own_rows // low_rows), zr), f32), V((nz, up8(2 * own_rows // low_rows), zr), f32),
            V((lw, zr), bf16), V((nz, 2 * own_rows, zr), bf16), V((2 * own_rows, 128), f32),
            V((n_t, 2, 2, rows, cols), bf16), V((2 * rows, n_t * cols), bf16), V((n_t, 2 * rows, 2 * cols), bf16),
            V((nz, n_t, nb, cr, cols), bf16), V((nz, group, cr, cols), bf16),
            V((nz, cr, cols), bf16), V((nz, cr, cols), bf16),
            V((2, 2, own, cols), f32), V((2, 2, own, cols), f32), V((2, own, cols), f32),
            V((nz * nb, cr, cols), bf16), V((2 * own_rows, cols), f32),
            V((own_rows, cols), bf16), V((own_rows, cols), bf16),
            V((2, half, cols), bf16), V((n_t - 1, 2, half, cols), bf16),
            V((2 * rows, half), f32), V((rows, half), bf16), V((rows, half), bf16),
            dma((8,)), dma((2, 8)), dma((2, n_t - 1)), dma((2, n_t - 1)),
            dma((2, n_t - 1, nb + 1)), dma((2, n_t - 1, 2, nb - 1)), dma((2, n_t - 1, nb + 1)),
            dma((2, nz, group)), dma((2, nz)), dma((2, nz, nb)),
        ],
        compiler_params=pltpu.CompilerParams(
            collective_id=0, has_side_effects=True, vmem_limit_bytes=48 * 1024 * 1024
        ),
    )(*(pltpu.with_memory_space_constraint(a, pltpu.HBM) for a in args))
    return pl.pallas_call(
        write_kernel,
        out_shape=(
            jax.ShapeDtypeStruct((rows, lw), bf16),
            jax.ShapeDtypeStruct((2, own, cols), f32),
            jax.ShapeDtypeStruct((2, own, cols), f32),
            jax.ShapeDtypeStruct((2, own_rows, cols), bf16),
        ),
        in_specs=[vmem] * 4,
        out_specs=(anywhere,) * 4,
        scratch_shapes=[dma((5,))],
        compiler_params=pltpu.CompilerParams(vmem_limit_bytes=8 * 1024 * 1024),
    )(ig, nf, ns, full)


def solution(mesh):
    in_specs = (
        P("dp", "tensor"),
        P(None, None, "tensor"),
        P(None, "dp", "tensor"),
        P(),
        P(),
        P(None, "dp", "tensor"),
        P(None, "dp", "tensor"),
    )
    out_specs = (
        P("dp", "tensor"),
        P(None, "dp", "tensor"),
        P(None, "dp", "tensor"),
        P(None, "dp", "tensor"),
    )
    return jax.shard_map(shards, mesh=mesh, in_specs=in_specs, out_specs=out_specs, check_vma=False)
```

```python
import functools
import math

import jax
import jax.numpy as jnp
from jax import lax
from jax.experimental import pallas as pl
from jax.experimental.pallas import tpu as pltpu
from jax.sharding import PartitionSpec as P

first_fix = 1.0 - 0.9**10
second_fix = 1.0 - 0.95**10
epsilon = 1e-08
bf16, f32 = jnp.bfloat16, jnp.float32
RELAY0 = 2


def wrap(value, period):
    return value & (period - 1) if period & (period - 1) == 0 else lax.rem(value, period)


def trig(phase, width):
    phase = wrap(phase, 4 * width)
    shift = width.bit_length() - 1
    quarter = (phase + width // 2) >> shift if 1 << shift == width else lax.div(phase + width // 2, width)
    x = (phase - quarter * width).astype(f32) * (math.pi / (2 * width))
    y = x * x
    c = 1.0 + y * (-0.5 + y * (1 / 24 + y * (-1 / 720 + y * (1 / 40320 - y * (1 / 3628800)))))
    s = x * (1.0 + y * (-1 / 6 + y * (1 / 120 + y * (-1 / 5040 + y * (1 / 362880)))))
    quarter = quarter & 3
    odd = (quarter & 1) == 1
    cosine = jnp.where(odd, s, c) * jnp.where((quarter == 1) | (quarter == 2), -1.0, 1.0)
    sine = jnp.where(odd, c, s) * jnp.where(quarter >= 2, -1.0, 1.0)
    return cosine, sine


def dot_last(a, b):
    return lax.dot_general(a, b, (((1,), (1,)), ((), ())), preferred_element_type=f32)


def main_kernel(
    plan,
    tok_ref, w_ref, hc_ref, freq_ref, sign_ref, first_ref, second_ref,
    ig_ref, nf_ref, ns_ref, full_ref,
    tok_all, tok_s, freq, sgn, sgn_b, cb, sb, ca, sa, ra, rb, back, sgn_col,
    hc_all, heads, pair_heads, quad_send, quad_recv, z_send, z_recv, mom, res, res_in, dirs, facc,
    f_send, f_recv, w_own, wp, g_acc, g_send, g_recv,
    loc, core_sems, tok_sems, hx_sems, hf_sems, wx_sems, wy_sems, wz_sems, quad_sems, z_sems, ag_sems,
):
    n_t, nz, nb, low_rows, token_count, width = plan
    rows, lw = tok_all.shape[1], tok_all.shape[2]
    rank = freq.shape[1]
    cr, cols = dirs.shape[1], dirs.shape[2]
    own = cr // 2
    zr = nb * cr
    own_rows = f_send.shape[0]
    half = lw // 2
    part = half // (2 * nb)
    piece = part // 2
    wide = min(512, half)
    deep = min(2048, lw)
    me_t, me_d = lax.axis_index("tensor"), lax.axis_index("dp")
    c, q = me_d % 2, me_d // 2
    y, z = q % nb, q // nb
    oc = 1 - c

    def dev(t, zz, yy, cc):
        return {"tensor": t, "dp": (zz * nb + yy) * 2 + cc}

    other = dev(me_t, z, y, oc)

    def xor(a, b):
        total, bit = 0, 1
        while bit < nz:
            total = total + bit * ((a // bit + b // bit) % 2)
            bit *= 2
        return total

    def remote(src, dst, send, recv, device):
        return pltpu.make_async_remote_copy(
            src_ref=src, dst_ref=dst, send_sem=send, recv_sem=recv,
            device_id=device, device_id_type=pl.DeviceIdType.MESH,
        )

    loads = [
        (freq_ref, freq),
        (tok_ref, tok_all.at[c]),
        (sign_ref.at[:, pl.ds(pl.multiple_of(me_t * lw, 128), lw)], sgn),
        (hc_ref, hc_all.at[me_t, c]),
        (sign_ref.at[:, pl.ds(pl.multiple_of(q * 2 * own_rows, 128), 2 * own_rows)], sgn_b),
        (first_ref.at[c], mom.at[0, c]),
        (second_ref.at[c], mom.at[1, c]),
        (w_ref.at[:, pl.ds(pl.multiple_of(me_t * lw + c * half, 128), half), :], w_own),
    ]
    loads = [pltpu.make_async_copy(a, b, loc.at[i]) for i, (a, b) in enumerate(loads)]
    for copy in loads:
        copy.start()

    barrier = pltpu.get_barrier_semaphore()
    peers = [other]
    for dt in range(n_t):
        for dy in range(nb):
            if dt or dy:
                peers.append(dev((me_t + dt) % n_t, z, (y + dy) % nb, c))
    for dt in range(1, n_t):
        peers.append(dev((me_t + dt) % n_t, z, y, oc))
    for s in range(1, nz):
        peers.append(dev(me_t, xor(z, s), y, c))
    for device in peers:
        pl.semaphore_signal(barrier, inc=1, device_id=device, device_id_type=pl.DeviceIdType.MESH)

    loads[0].wait()
    f = jnp.where(c == 0, freq[0:1, :], freq[1:2, :])
    scale = jnp.where(f == 0, math.sqrt(1.0 / width), math.sqrt(2.0 / width)).astype(f32)

    def fill(cos_ref, sin_ref, start, stride, scaled):
        def block(r, carry):
            index = r * 8 + lax.broadcasted_iota(jnp.int32, (8, rank), 0)
            cosine, sine = trig((start + stride * index) * f, width)
            if scaled:
                cosine, sine = cosine * scale, sine * scale
            place = pl.ds(pl.multiple_of(r * 8, 8), 8)
            for k in range(nz):
                cos_ref[k, place, :] = cosine[:, k * zr : (k + 1) * zr]
                sin_ref[k, place, :] = sine[:, k * zr : (k + 1) * zr]
            return carry

        lax.fori_loop(0, cos_ref.shape[1] // 8, block, 0)

    fill(cb, sb, 1, 2, False)
    pl.semaphore_wait(barrier, len(peers))

    early = [
        remote(hc_ref, hc_all.at[me_t, c], core_sems.at[0, 0], core_sems.at[1, 0], other),
        remote(first_ref.at[oc], mom.at[0, c], core_sems.at[0, 1], core_sems.at[1, 1], other),
        remote(second_ref.at[oc], mom.at[1, c], core_sems.at[0, 2], core_sems.at[1, 2], other),
    ]

    def tensor_peer(s):
        return dev((me_t + s) % n_t, z, y, c)

    def hx_copy(s, k):
        m = (c + k) % 2
        return remote(
            hc_ref.at[m], hc_all.at[me_t, c, m], hx_sems.at[0, s - 1, k], hx_sems.at[1, s - 1, k],
            dev((me_t + s) % n_t, z, y, m),
        )

    def hf_copy(s):
        slot = hc_all.at[(me_t + n_t - s) % n_t, :, c]
        return remote(slot, slot, hf_sems.at[0, s - 1], hf_sems.at[1, s - 1], other)

    def tok_copy(p):
        place = slice(p * (lw // 4), (p + 1) * (lw // 4))
        return remote(
            tok_ref.at[:, place], tok_all.at[c, :, place], tok_sems.at[0, p], tok_sems.at[1, p], other
        )

    def rows_of(yy, zl, p):
        return pl.multiple_of((yy * 2 + zl) * part + p * piece, 16)

    zl = z % 2

    def wx_copy(s, k):
        yy, zz, p = (y, zl, k) if k < 2 else ((y + k - 1) % nb, 1 - zl, 1)
        row = rows_of(yy, zz, p)
        at = pl.ds(pl.multiple_of(((me_t + s) % n_t) * lw + c * half + row, 16), piece)
        return remote(
            w_ref.at[:, at, :], wp.at[s - 1, :, pl.ds(row, piece), :],
            wx_sems.at[0, s - 1, k], wx_sems.at[1, s - 1, k], tensor_peer(s),
        )

    def wy_copy(s, p, dy):
        slot = wp.at[s - 1, :, pl.ds(rows_of(y, zl, p), piece), :]
        return remote(
            slot, slot, wy_sems.at[0, s - 1, p, dy - 1], wy_sems.at[1, s - 1, p, dy - 1],
            dev(me_t, z, (y + dy) % nb, c),
        )

    def wz_copy(s, k):
        yy, p = (y, k) if k < 2 else ((y + nb - (k - 1)) % nb, 0)
        slot = wp.at[s - 1, :, pl.ds(rows_of(yy, zl, p), piece), :]
        return remote(
            slot, slot, wz_sems.at[0, s - 1, k], wz_sems.at[1, s - 1, k], dev(me_t, xor(z, 1), y, c)
        )

    tensor_peers, y_peers = range(1, n_t), range(1, nb)

    def fetch(k):
        for s in tensor_peers:
            wx_copy(s, k).start()

    def relay(p):
        for s in tensor_peers:
            wx_copy(s, p).wait_recv()
            for dy in y_peers:
                wy_copy(s, p, dy).start()
            wz_copy(s, p).start()

    def forward():
        for s in tensor_peers:
            for dy in y_peers:
                wy_copy(s, 0, dy).wait_recv()
                wz_copy(s, 1 + dy).start()

    for s in range(1, n_t):
        for k in range(2):
            hx_copy(s, k).start()
    for p in range(4):
        tok_copy(p).start()
    for copy in early:
        copy.start()
    fetch(0)
    fetch(1)

    fill(ca, sa, 2 * me_t * lw, 2 * low_rows, True)

    def sign_tokens(k, start, count):
        for j in range(start, start + count, count // 2):
            place = slice(j, j + count // 2)
            row = jnp.where(c == 0, sgn[0:1, place], sgn[1:2, place])
            row = (2 * row - 1).astype(f32).astype(bf16)
            tok_s[pl.ds(k, 1), :, place] = tok_all[pl.ds(k, 1), :, place] * row

    loads[1].wait()
    loads[2].wait()
    for p in range(4):
        sign_tokens(c, p * (lw // 4), lw // 4)

    def tables(a_ref, b_ref, h, k):
        row = pl.ds(h, 1)
        return (a_ref[k, row, :] * cb[k] - b_ref[k, row, :] * sb[k]).astype(bf16)

    def quad_copy(i, dt, dy):
        slot = dt * nb + dy - 1
        t, yy = (me_t + dt) % n_t, (y + dy) % nb
        return remote(
            quad_send.at[i, t, yy], quad_recv.at[i, slot],
            quad_sems.at[0, i, slot], quad_sems.at[1, i, slot], dev(t, z, yy, c),
        )

    quad_slots = [(dt, dy) for dt in range(n_t) for dy in range(nb) if dt or dy]

    def z_copy(i):
        return remote(
            z_send.at[i], z_recv.at[i], z_sems.at[0, i], z_sems.at[1, i], dev(me_t, xor(z, nz - 1 - i), y, c)
        )

    def reduced(i):
        total = quad_send[i, me_t, y].astype(f32)
        for dt, dy in quad_slots:
            quad_copy(i, dt, dy).wait_recv()
            total = total + quad_recv[i, dt * nb + dy - 1].astype(f32)
        return total

    def pass_on(i):
        z_send[i] = reduced(i).astype(bf16)
        z_copy(i).start()

    def project(k, step, ready):
        projected = 0.0
        for j in range(0, lw, step):
            ready(j)
            basis = jnp.concatenate([tables(ca, sa, (j + h) // low_rows, k) for h in range(0, step, low_rows)], axis=0)
            signed = tok_s[:, :, j : j + step].reshape(2 * rows, step)
            projected = projected + jnp.dot(signed, basis, preferred_element_type=f32)
        return projected.astype(bf16)

    def low_rank(i, projected):
        low = lax.dot_general(
            projected, heads[...], (((0,), (0,)), ((), ())), preferred_element_type=f32
        ).astype(bf16)
        for t in range(n_t):
            for yy in range(nb):
                quad_send[i, t, yy] = low[yy * cr : (yy + 1) * cr, t * cols : (t + 1) * cols]
        for dt, dy in quad_slots:
            quad_copy(i, dt, dy).start()

    def arrive(j):
        tok_copy(j // (lw // 4)).wait_recv()
        sign_tokens(oc, j, lw // 4)

    projected = project(xor(z, nz - 1), lw // 4, arrive)
    loads[3].wait()
    early[0].wait_recv()
    for s in tensor_peers:
        for k in range(2):
            hx_copy(s, k).wait_recv()
    for t in range(n_t):
        heads[:, t * cols : (t + 1) * cols] = hc_all[t, :, pl.ds(c, 1)].reshape(2 * rows, cols)
    low_rank(0, projected)
    for s in tensor_peers:
        hf_copy(s).start()

    def chunk(i, carry):
        low_rank(i, project(xor(z, nz - 1 - i), deep, lambda j: None))
        return carry

    lax.fori_loop(1, nz, chunk, 0)

    relay(0)
    for i in range(nz - 1):
        pass_on(i)
    fill(ra, rb, 2 * q * 2 * own_rows, 2 * low_rows, True)
    def back_rows(h, carry):
        place = pl.ds(pl.multiple_of(h * low_rows, low_rows), low_rows)
        for k in range(nz):
            back[k, place, :] = tables(ra, rb, h, k)
        return carry

    lax.fori_loop(0, back.shape[1] // low_rows, back_rows, 0)
    loads[4].wait()
    lane = min(128, 2 * own_rows)
    for b in range(2 * own_rows // lane):
        at = slice(b * lane, (b + 1) * lane)
        row = (2 * jnp.where(c == 0, sgn_b[0:1, at], sgn_b[1:2, at]) - 1).astype(f32)
        sgn_col[b * lane : (b + 1) * lane, :] = jnp.broadcast_to(row, (128, lane)).T
    loads[7].wait()
    for s in tensor_peers:
        hf_copy(s).wait_recv()
    for t in range(n_t):
        for m in range(2):
            pair_heads[t, :, m * cols : (m + 1) * cols] = hc_all[t, :, m].reshape(2 * rows, cols)

    def own_gradient(j, carry):
        place = pl.ds(pl.multiple_of(j * wide, wide), wide)
        w = jnp.concatenate([w_own[m, place, :] for m in range(2)], axis=1)
        g_acc[:, place] = dot_last(pair_heads[me_t], w)
        return carry

    lax.fori_loop(0, half // wide, own_gradient, 0)
    relay(1)
    for i in (5, 6):
        loads[i].wait()
    for i in (1, 2):
        early[i].wait_recv()

    total = reduced(nz - 1)
    for k in range(2, nb + 1):
        fetch(k)
    for i in range(nz - 1):
        z_copy(i).wait_recv()
        total = total + z_recv[i].astype(f32)
    gradient = (total / math.sqrt(token_count)).reshape(2, own, cols)
    new_first = 0.9 * mom[0] + 0.1 * gradient
    new_second = 0.95 * mom[1] + 0.05 * gradient * gradient
    direction = new_first / first_fix / (jnp.sqrt(new_second / second_fix) + epsilon)
    dirs[pl.ds(z * nb + y, 1)] = direction.astype(bf16).reshape(1, cr, cols)

    def ag_copy(s, dy):
        if dy == 0:
            slot = dirs.at[z * nb + y]
            return remote(slot, slot, ag_sems.at[0, s, 0], ag_sems.at[1, s, 0], dev(me_t, xor(z, s), y, c))
        slot = dirs.at[xor(z, s) * nb + y]
        return remote(
            slot, slot, ag_sems.at[0, s, dy], ag_sems.at[1, s, dy], dev(me_t, z, (y + dy) % nb, c)
        )

    for s in range(nz - 1, 0, -1):
        ag_copy(s, 0).start()
    for dy in range(1, nb):
        ag_copy(0, dy).start()
    res[0] = new_first
    res[1] = new_second
    res_copies = [
        remote(res.at[k, oc], res_in.at[k], core_sems.at[0, 3 + k], core_sems.at[1, 3 + k], other)
        for k in range(2)
    ]
    for copy in res_copies:
        copy.start()

    forward()
    for s in range(1, nz):
        ag_copy(s, 0).wait_recv()
        for dy in range(1, nb):
            ag_copy(s, dy).start()
    for s in tensor_peers:
        for dy in y_peers:
            wy_copy(s, 1, dy).wait_recv()
            wx_copy(s, 1 + dy).wait_recv()
        for k in range(nb + 1):
            wz_copy(s, k).wait_recv()

    def add_gradient(j, carry):
        place = pl.ds(pl.multiple_of(j * wide, wide), wide)
        value = g_acc[:, place]
        for s in range(1, n_t):
            w = jnp.concatenate([wp[s - 1, m, place, :] for m in range(2)], axis=1)
            value = value + dot_last(pair_heads[(me_t + n_t - s) % n_t], w)
        g_acc[:, place] = value
        g_send[:, place] = g_acc[pl.ds(pl.multiple_of(oc * rows, rows), rows), place].astype(bf16)
        mine = g_acc[pl.ds(pl.multiple_of(c * rows, rows), rows), place].astype(bf16)
        ig_ref[pl.ds(c, 1), :, place] = mine[None]
        return carry

    lax.fori_loop(0, half // wide, add_gradient, 0)
    g_copy = remote(g_send, g_recv, core_sems.at[0, 6], core_sems.at[1, 6], other)
    g_copy.start()

    nf_ref[pl.ds(c, 1)] = res[0, pl.ds(c, 1)]
    ns_ref[pl.ds(c, 1)] = res[1, pl.ds(c, 1)]
    for copy in res_copies:
        copy.wait_recv()
    nf_ref[pl.ds(oc, 1)] = res_in[0][None]
    ns_ref[pl.ds(oc, 1)] = res_in[1][None]
    facc[...] = jnp.zeros_like(facc)
    for s in range(nz):
        for dy in range(1, nb):
            ag_copy(s, dy).wait_recv()
        zz = xor(z, s)
        block = dirs[pl.ds(zz * nb, nb)].reshape(zr, cols)
        facc[...] += jnp.dot(back[zz], block, preferred_element_type=f32)

    def finished(k):
        place = pl.ds(pl.multiple_of(k * own_rows, own_rows), own_rows)
        value, signs = facc[place, :], sgn_col[place, :]
        return jnp.concatenate(
            [value[:, j : j + 128] * signs for j in range(0, cols, 128)], axis=1
        ).astype(bf16)

    f_send[...] = finished(oc)
    f_copy = remote(f_send, f_recv, core_sems.at[0, 5], core_sems.at[1, 5], other)
    f_copy.start()
    full_ref[pl.ds(c, 1)] = finished(c)[None]

    for copy in (g_copy, f_copy):
        copy.wait_recv()
    ig_ref[pl.ds(oc, 1)] = g_recv[...][None]
    full_ref[pl.ds(oc, 1)] = f_recv[...][None]

    for p in range(4):
        tok_copy(p).wait_send()
    for copy in early + res_copies + [f_copy, g_copy]:
        copy.wait_send()
    for s in range(1, n_t):
        for k in range(2):
            hx_copy(s, k).wait_send()
        hf_copy(s).wait_send()
        for k in range(nb + 1):
            wx_copy(s, k).wait_send()
            wz_copy(s, k).wait_send()
        for dy in y_peers:
            for p in range(2):
                wy_copy(s, p, dy).wait_send()

    def sent(i, carry):
        for dt, dy in quad_slots:
            quad_copy(i, dt, dy).wait_send()
        return carry

    lax.fori_loop(0, nz, sent, 0)
    for i in range(nz - 1):
        z_copy(i).wait_send()
    for s in range(nz):
        for dy in range(nb):
            if s or dy:
                ag_copy(s, dy).wait_send()


def write_kernel(ig, nf, ns, full, ig_out, nf_out, ns_out, full_out, sems):
    half = ig.shape[2]
    copies = [(ig.at[k], ig_out.at[:, k * half : (k + 1) * half]) for k in range(2)]
    copies += [(full, full_out), (nf, nf_out), (ns, ns_out)]
    copies = [pltpu.make_async_copy(a, b, sems.at[i]) for i, (a, b) in enumerate(copies)]
    for copy in copies:
        copy.start()
    for copy in copies:
        copy.wait()


def shards(
    tokens, projection_weights, head_cotangent, frequencies, sign_bits, first_moment, second_moment
):
    rows, lw = tokens.shape
    n_t, n_dp = lax.axis_size("tensor"), lax.axis_size("dp")
    width = lw * n_t
    rank = frequencies.shape[1]
    own, cols = first_moment.shape[1], first_moment.shape[2]
    own_rows = projection_weights.shape[1] // n_dp
    chips = n_dp // 2
    cr = 2 * own
    nb = 2
    while nb * cr % 128:
        nb *= 2
    nz = chips // nb
    zr = nb * cr
    low_rows = min(128, 2 * own_rows)
    up8 = lambda n: -(-n // 8) * 8
    half = lw // 2
    group = n_t * nb - 1

    anywhere, vmem = pl.BlockSpec(memory_space=pltpu.HBM), pl.BlockSpec(memory_space=pltpu.VMEM)
    dma = pltpu.SemaphoreType.DMA
    V = pltpu.VMEM
    args = (tokens, projection_weights, head_cotangent, frequencies, sign_bits, first_moment, second_moment)
    plan = (n_t, nz, nb, low_rows, rows * n_dp, width)
    ig, nf, ns, full = pl.pallas_call(
        functools.partial(main_kernel, plan),
        out_shape=(
            jax.ShapeDtypeStruct((2, rows, half), bf16),
            jax.ShapeDtypeStruct((2, own, cols), f32),
            jax.ShapeDtypeStruct((2, own, cols), f32),
            jax.ShapeDtypeStruct((2, own_rows, cols), bf16),
        ),
        in_specs=[anywhere] * 7,
        out_specs=(vmem,) * 4,
        scratch_shapes=[
            V((2, rows, lw), bf16), V((2, rows, lw), bf16), V((2, rank), jnp.int32),
            V((2, lw), jnp.int32), V((2, 2 * own_rows), jnp.int32),
            V((nz, low_rows, zr), f32), V((nz, low_rows, zr), f32),
            V((nz, up8(lw // low_rows), zr), f32), V((nz, up8(lw // low_rows), zr), f32),
            V((nz, up8(2 * own_rows // low_rows), zr), f32), V((nz, up8(2 * own_rows // low_rows), zr), f32),
            V((nz, 2 * own_rows, zr), bf16), V((2 * own_rows, 128), f32),
            V((n_t, 2, 2, rows, cols), bf16), V((2 * rows, n_t * cols), bf16), V((n_t, 2 * rows, 2 * cols), bf16),
            V((nz, n_t, nb, cr, cols), bf16), V((nz, group, cr, cols), bf16),
            V((nz, cr, cols), bf16), V((nz, cr, cols), bf16),
            V((2, 2, own, cols), f32), V((2, 2, own, cols), f32), V((2, own, cols), f32),
            V((nz * nb, cr, cols), bf16), V((2 * own_rows, cols), f32),
            V((own_rows, cols), bf16), V((own_rows, cols), bf16),
            V((2, half, cols), bf16), V((n_t - 1, 2, half, cols), bf16),
            V((2 * rows, half), f32), V((rows, half), bf16), V((rows, half), bf16),
            dma((8,)), dma((2, 7)), dma((2, 4)), dma((2, n_t - 1, 2)), dma((2, n_t - 1)),
            dma((2, n_t - 1, nb + 1)), dma((2, n_t - 1, 2, nb - 1)), dma((2, n_t - 1, nb + 1)),
            dma((2, nz, group)), dma((2, nz)), dma((2, nz, nb)),
        ],
        compiler_params=pltpu.CompilerParams(
            collective_id=0, has_side_effects=True, vmem_limit_bytes=48 * 1024 * 1024
        ),
    )(*(pltpu.with_memory_space_constraint(a, pltpu.HBM) for a in args))
    return pl.pallas_call(
        write_kernel,
        out_shape=(
            jax.ShapeDtypeStruct((rows, lw), bf16),
            jax.ShapeDtypeStruct((2, own, cols), f32),
            jax.ShapeDtypeStruct((2, own, cols), f32),
            jax.ShapeDtypeStruct((2, own_rows, cols), bf16),
        ),
        in_specs=[vmem] * 4,
        out_specs=(anywhere,) * 4,
        scratch_shapes=[dma((5,))],
        compiler_params=pltpu.CompilerParams(vmem_limit_bytes=8 * 1024 * 1024),
    )(ig, nf, ns, full)


def solution(mesh):
    in_specs = (
        P("dp", "tensor"),
        P(None, None, "tensor"),
        P(None, "dp", "tensor"),
        P(),
        P(),
        P(None, "dp", "tensor"),
        P(None, "dp", "tensor"),
    )
    out_specs = (
        P("dp", "tensor"),
        P(None, "dp", "tensor"),
        P(None, "dp", "tensor"),
        P(None, "dp", "tensor"),
    )
    return jax.shard_map(shards, mesh=mesh, in_specs=in_specs, out_specs=out_specs, check_vma=False)
```

```python
import functools
import math

import jax
import jax.numpy as jnp
from jax import lax
from jax.experimental import pallas as pl
from jax.experimental.pallas import tpu as pltpu
from jax.sharding import PartitionSpec as P

first_fix = 1.0 - 0.9**10
second_fix = 1.0 - 0.95**10
epsilon = 1e-08
bf16, f32 = jnp.bfloat16, jnp.float32
RELAY0 = 2


def wrap(value, period):
    return value & (period - 1) if period & (period - 1) == 0 else lax.rem(value, period)


def trig(phase, width):
    phase = wrap(phase, 4 * width)
    shift = width.bit_length() - 1
    quarter = (phase + width // 2) >> shift if 1 << shift == width else lax.div(phase + width // 2, width)
    x = (phase - quarter * width).astype(f32) * (math.pi / (2 * width))
    y = x * x
    c = 1.0 + y * (-0.5 + y * (1 / 24 + y * (-1 / 720 + y * (1 / 40320 - y * (1 / 3628800)))))
    s = x * (1.0 + y * (-1 / 6 + y * (1 / 120 + y * (-1 / 5040 + y * (1 / 362880)))))
    quarter = quarter & 3
    odd = (quarter & 1) == 1
    cosine = jnp.where(odd, s, c) * jnp.where((quarter == 1) | (quarter == 2), -1.0, 1.0)
    sine = jnp.where(odd, c, s) * jnp.where(quarter >= 2, -1.0, 1.0)
    return cosine, sine


def dot_last(a, b):
    return lax.dot_general(a, b, (((1,), (1,)), ((), ())), preferred_element_type=f32)


def main_kernel(
    plan,
    tok_ref, w_ref, hc_ref, freq_ref, sign_ref, first_ref, second_ref,
    ig_ref, nf_ref, ns_ref, full_ref,
    tok_all, tok_s, freq, sgn, sgn_b, cb, sb, ca, sa, ra, rb, back, sgn_col,
    hc_all, heads, pair_heads, y_send, y_recv, x_send, x_recv, z_send, z_recv, mom, res, res_in, dirs, facc,
    f_send, f_recv, w_own, wp, g_acc, g_send, g_recv,
    loc, core_sems, tok_sems, hx_sems, hf_sems, wx_sems, wy_sems, wz_sems, y_sems, x_sems, z_sems, ag_sems,
):
    n_t, nz, nb, low_rows, token_count, width = plan
    rows, lw = tok_all.shape[1], tok_all.shape[2]
    rank = freq.shape[1]
    cr, cols = dirs.shape[1], dirs.shape[2]
    own = cr // 2
    zr = nb * cr
    own_rows = f_send.shape[0]
    half = lw // 2
    part = half // (2 * nb)
    piece = part // 2
    wide = min(512, half)
    deep = min(2048, lw)
    me_t, me_d = lax.axis_index("tensor"), lax.axis_index("dp")
    c, q = me_d % 2, me_d // 2
    y, z = q % nb, q // nb
    oc = 1 - c

    def dev(t, zz, yy, cc):
        return {"tensor": t, "dp": (zz * nb + yy) * 2 + cc}

    other = dev(me_t, z, y, oc)

    def xor(a, b):
        total, bit = 0, 1
        while bit < nz:
            total = total + bit * ((a // bit + b // bit) % 2)
            bit *= 2
        return total

    def remote(src, dst, send, recv, device):
        return pltpu.make_async_remote_copy(
            src_ref=src, dst_ref=dst, send_sem=send, recv_sem=recv,
            device_id=device, device_id_type=pl.DeviceIdType.MESH,
        )

    loads = [
        (freq_ref, freq),
        (tok_ref, tok_all.at[c]),
        (sign_ref.at[:, pl.ds(pl.multiple_of(me_t * lw, 128), lw)], sgn),
        (hc_ref, hc_all.at[me_t, c]),
        (sign_ref.at[:, pl.ds(pl.multiple_of(q * 2 * own_rows, 128), 2 * own_rows)], sgn_b),
        (first_ref.at[c], mom.at[0, c]),
        (second_ref.at[c], mom.at[1, c]),
        (w_ref.at[:, pl.ds(pl.multiple_of(me_t * lw + c * half, 128), half), :], w_own),
    ]
    loads = [pltpu.make_async_copy(a, b, loc.at[i]) for i, (a, b) in enumerate(loads)]
    for copy in loads:
        copy.start()

    barrier = pltpu.get_barrier_semaphore()
    peers = [other]
    for dy in range(1, nb):
        peers.append(dev(me_t, z, (y + dy) % nb, c))
    for dt in range(1, n_t):
        peers += [dev((me_t + dt) % n_t, z, y, c), dev((me_t + dt) % n_t, z, y, oc)]
    for s in range(1, nz):
        peers.append(dev(me_t, xor(z, s), y, c))
    for device in peers:
        pl.semaphore_signal(barrier, inc=1, device_id=device, device_id_type=pl.DeviceIdType.MESH)

    loads[0].wait()
    f = jnp.where(c == 0, freq[0:1, :], freq[1:2, :])
    scale = jnp.where(f == 0, math.sqrt(1.0 / width), math.sqrt(2.0 / width)).astype(f32)

    def fill(cos_ref, sin_ref, start, stride, scaled):
        def block(r, carry):
            index = r * 8 + lax.broadcasted_iota(jnp.int32, (8, rank), 0)
            cosine, sine = trig((start + stride * index) * f, width)
            if scaled:
                cosine, sine = cosine * scale, sine * scale
            place = pl.ds(pl.multiple_of(r * 8, 8), 8)
            for k in range(nz):
                cos_ref[k, place, :] = cosine[:, k * zr : (k + 1) * zr]
                sin_ref[k, place, :] = sine[:, k * zr : (k + 1) * zr]
            return carry

        lax.fori_loop(0, cos_ref.shape[1] // 8, block, 0)

    fill(cb, sb, 1, 2, False)
    pl.semaphore_wait(barrier, len(peers))

    early = [
        remote(hc_ref, hc_all.at[me_t, c], core_sems.at[0, 0], core_sems.at[1, 0], other),
        remote(first_ref.at[oc], mom.at[0, c], core_sems.at[0, 1], core_sems.at[1, 1], other),
        remote(second_ref.at[oc], mom.at[1, c], core_sems.at[0, 2], core_sems.at[1, 2], other),
    ]

    def tensor_peer(s):
        return dev((me_t + s) % n_t, z, y, c)

    def hx_copy(s, k):
        m = (c + k) % 2
        return remote(
            hc_ref.at[m], hc_all.at[me_t, c, m], hx_sems.at[0, s - 1, k], hx_sems.at[1, s - 1, k],
            dev((me_t + s) % n_t, z, y, m),
        )

    def hf_copy(s):
        slot = hc_all.at[(me_t + n_t - s) % n_t, :, c]
        return remote(slot, slot, hf_sems.at[0, s - 1], hf_sems.at[1, s - 1], other)

    def tok_copy(p):
        place = slice(p * (lw // 4), (p + 1) * (lw // 4))
        return remote(
            tok_ref.at[:, place], tok_all.at[c, :, place], tok_sems.at[0, p], tok_sems.at[1, p], other
        )

    def rows_of(yy, zl, p):
        return pl.multiple_of((yy * 2 + zl) * part + p * piece, 16)

    zl = z % 2

    def wx_copy(s, k):
        yy, zz = (y, zl) if k < 2 else ((y + k // 2) % nb, 1 - zl)
        row = rows_of(yy, zz, k % 2)
        at = pl.ds(pl.multiple_of(((me_t + s) % n_t) * lw + c * half + row, 16), piece)
        return remote(
            w_ref.at[:, at, :], wp.at[s - 1, :, pl.ds(row, piece), :],
            wx_sems.at[0, s - 1, k], wx_sems.at[1, s - 1, k], tensor_peer(s),
        )

    def wy_copy(s, p, dy):
        slot = wp.at[s - 1, :, pl.ds(rows_of(y, zl, p), piece), :]
        return remote(
            slot, slot, wy_sems.at[0, s - 1, p, dy - 1], wy_sems.at[1, s - 1, p, dy - 1],
            dev(me_t, z, (y + dy) % nb, c),
        )

    def wz_copy(s, p):
        slot = wp.at[s - 1, :, pl.ds(rows_of(y, zl, p), piece), :]
        return remote(
            slot, slot, wz_sems.at[0, s - 1, p], wz_sems.at[1, s - 1, p], dev(me_t, xor(z, 1), y, c)
        )

    tensor_peers, y_peers = range(1, n_t), range(1, nb)

    def fetch(k):
        for s in tensor_peers:
            wx_copy(s, k).start()

    def relay_z(p):
        for s in tensor_peers:
            wx_copy(s, p).wait_recv()
            wz_copy(s, p).start()

    def relay_y(p):
        for s in tensor_peers:
            for dy in y_peers:
                wy_copy(s, p, dy).start()

    for s in range(1, n_t):
        for k in range(2):
            hx_copy(s, k).start()
    for p in range(4):
        tok_copy(p).start()
    for copy in early:
        copy.start()
    fetch(0)
    fetch(1)

    fill(ca, sa, 2 * me_t * lw, 2 * low_rows, True)

    def sign_tokens(k, start, count):
        for j in range(start, start + count, count // 2):
            place = slice(j, j + count // 2)
            row = jnp.where(c == 0, sgn[0:1, place], sgn[1:2, place])
            row = (2 * row - 1).astype(f32).astype(bf16)
            tok_s[pl.ds(k, 1), :, place] = tok_all[pl.ds(k, 1), :, place] * row

    loads[1].wait()
    loads[2].wait()
    for p in range(4):
        sign_tokens(c, p * (lw // 4), lw // 4)

    def tables(a_ref, b_ref, h, k):
        row = pl.ds(h, 1)
        return (a_ref[k, row, :] * cb[k] - b_ref[k, row, :] * sb[k]).astype(bf16)

    def y_copy(i, dy):
        yy = (y + dy) % nb
        return remote(
            y_send.at[i, yy], y_recv.at[i, dy - 1], y_sems.at[0, i, dy - 1], y_sems.at[1, i, dy - 1],
            dev(me_t, z, yy, c),
        )

    def x_copy(i, s):
        return remote(
            x_send.at[i, (me_t + s) % n_t], x_recv.at[i, s - 1],
            x_sems.at[0, i, s - 1], x_sems.at[1, i, s - 1], tensor_peer(s),
        )

    def z_copy(i):
        return remote(
            z_send.at[i], z_recv.at[i], z_sems.at[0, i], z_sems.at[1, i], dev(me_t, xor(z, nz - 1 - i), y, c)
        )

    def over_y(i):
        total = y_send[i, y].astype(f32)
        for dy in y_peers:
            y_copy(i, dy).wait_recv()
            total = total + y_recv[i, dy - 1].astype(f32)
        total = total.astype(bf16)
        for t in range(n_t):
            x_send[i, t] = total[:, t * cols : (t + 1) * cols]
        for s in tensor_peers:
            x_copy(i, s).start()

    def over_x(i):
        total = x_send[i, me_t].astype(f32)
        for s in tensor_peers:
            x_copy(i, s).wait_recv()
            total = total + x_recv[i, s - 1].astype(f32)
        return total

    def project(k, step, ready):
        projected = 0.0
        for j in range(0, lw, step):
            ready(j)
            basis = jnp.concatenate([tables(ca, sa, (j + h) // low_rows, k) for h in range(0, step, low_rows)], axis=0)
            signed = tok_s[:, :, j : j + step].reshape(2 * rows, step)
            projected = projected + jnp.dot(signed, basis, preferred_element_type=f32)
        return projected.astype(bf16)

    def low_rank(i, projected):
        low = lax.dot_general(
            projected, heads[...], (((0,), (0,)), ((), ())), preferred_element_type=f32
        ).astype(bf16)
        for yy in range(nb):
            y_send[i, yy] = low[yy * cr : (yy + 1) * cr, :]
        for dy in y_peers:
            y_copy(i, dy).start()

    def arrive(j):
        tok_copy(j // (lw // 4)).wait_recv()
        sign_tokens(oc, j, lw // 4)

    projected = project(xor(z, nz - 1), lw // 4, arrive)
    loads[3].wait()
    early[0].wait_recv()
    for s in tensor_peers:
        for k in range(2):
            hx_copy(s, k).wait_recv()
    for t in range(n_t):
        heads[:, t * cols : (t + 1) * cols] = hc_all[t, :, pl.ds(c, 1)].reshape(2 * rows, cols)
    low_rank(0, projected)
    for s in tensor_peers:
        hf_copy(s).start()

    def chunk(i, carry):
        low_rank(i, project(xor(z, nz - 1 - i), deep, lambda j: None))

        @pl.when(i == RELAY0)
        def _():
            relay_z(0)

        return carry

    lax.fori_loop(1, nz, chunk, 0)

    def back_rows(h, carry):
        place = pl.ds(pl.multiple_of(h * low_rows, low_rows), low_rows)
        for k in range(nz):
            back[k, place, :] = tables(ra, rb, h, k)
        return carry

    def fill_back():
        fill(ra, rb, 2 * q * 2 * own_rows, 2 * low_rows, True)
        for s in tensor_peers:
            hf_copy(s).wait_recv()
        for t in range(n_t):
            for m in range(2):
                pair_heads[t, :, m * cols : (m + 1) * cols] = hc_all[t, :, m].reshape(2 * rows, cols)

    def build_back():
        lax.fori_loop(0, back.shape[1] // low_rows, back_rows, 0)

    def column_signs():
        loads[4].wait()
        lane = min(128, 2 * own_rows)
        for b in range(2 * own_rows // lane):
            at = slice(b * lane, (b + 1) * lane)
            row = (2 * jnp.where(c == 0, sgn_b[0:1, at], sgn_b[1:2, at]) - 1).astype(f32)
            sgn_col[b * lane : (b + 1) * lane, :] = jnp.broadcast_to(row, (128, lane)).T

    def own_gradient(j, carry):
        place = pl.ds(pl.multiple_of(j * wide, wide), wide)
        w = jnp.concatenate([w_own[m, place, :] for m in range(2)], axis=1)
        g_acc[:, place] = dot_last(pair_heads[me_t], w)
        return carry

    fillers = {0: fill_back, 1: build_back, 2: column_signs}
    for i in range(nz):
        over_y(i)
        if i == 1:
            relay_z(1)
        if i in fillers:
            fillers[i]()
        if i:
            z_send[i - 1] = over_x(i - 1).astype(bf16)
            z_copy(i - 1).start()
    relay_y(0)
    relay_y(1)
    loads[7].wait()
    lax.fori_loop(0, half // wide, own_gradient, 0)
    for i in (5, 6):
        loads[i].wait()
    for i in (1, 2):
        early[i].wait_recv()

    total = over_x(nz - 1)
    for k in range(2, 2 * nb):
        fetch(k)
    for i in range(nz - 1):
        z_copy(i).wait_recv()
        total = total + z_recv[i].astype(f32)
    gradient = (total / math.sqrt(token_count)).reshape(2, own, cols)
    new_first = 0.9 * mom[0] + 0.1 * gradient
    new_second = 0.95 * mom[1] + 0.05 * gradient * gradient
    direction = new_first / first_fix / (jnp.sqrt(new_second / second_fix) + epsilon)
    dirs[pl.ds(z * nb + y, 1)] = direction.astype(bf16).reshape(1, cr, cols)

    def ag_copy(s, dy):
        if dy == 0:
            slot = dirs.at[z * nb + y]
            return remote(slot, slot, ag_sems.at[0, s, 0], ag_sems.at[1, s, 0], dev(me_t, xor(z, s), y, c))
        slot = dirs.at[xor(z, s) * nb + y]
        return remote(
            slot, slot, ag_sems.at[0, s, dy], ag_sems.at[1, s, dy], dev(me_t, z, (y + dy) % nb, c)
        )

    for s in range(nz - 1, 0, -1):
        ag_copy(s, 0).start()
    for dy in range(1, nb):
        ag_copy(0, dy).start()
    res[0] = new_first
    res[1] = new_second
    res_copies = [
        remote(res.at[k, oc], res_in.at[k], core_sems.at[0, 3 + k], core_sems.at[1, 3 + k], other)
        for k in range(2)
    ]
    for copy in res_copies:
        copy.start()

    for s in range(1, nz):
        ag_copy(s, 0).wait_recv()
        for dy in range(1, nb):
            ag_copy(s, dy).start()
    for s in tensor_peers:
        for k in range(2, 2 * nb):
            wx_copy(s, k).wait_recv()
        for p in range(2):
            wz_copy(s, p).wait_recv()
            for dy in y_peers:
                wy_copy(s, p, dy).wait_recv()

    def add_gradient(j, carry):
        place = pl.ds(pl.multiple_of(j * wide, wide), wide)
        value = g_acc[:, place]
        for s in range(1, n_t):
            w = jnp.concatenate([wp[s - 1, m, place, :] for m in range(2)], axis=1)
            value = value + dot_last(pair_heads[(me_t + n_t - s) % n_t], w)
        g_acc[:, place] = value
        g_send[:, place] = g_acc[pl.ds(pl.multiple_of(oc * rows, rows), rows), place].astype(bf16)
        mine = g_acc[pl.ds(pl.multiple_of(c * rows, rows), rows), place].astype(bf16)
        ig_ref[pl.ds(c, 1), :, place] = mine[None]
        return carry

    lax.fori_loop(0, half // wide, add_gradient, 0)
    g_copy = remote(g_send, g_recv, core_sems.at[0, 6], core_sems.at[1, 6], other)
    g_copy.start()

    nf_ref[pl.ds(c, 1)] = res[0, pl.ds(c, 1)]
    ns_ref[pl.ds(c, 1)] = res[1, pl.ds(c, 1)]
    for copy in res_copies:
        copy.wait_recv()
    nf_ref[pl.ds(oc, 1)] = res_in[0][None]
    ns_ref[pl.ds(oc, 1)] = res_in[1][None]
    facc[...] = jnp.zeros_like(facc)
    for s in range(nz):
        for dy in range(1, nb):
            ag_copy(s, dy).wait_recv()
        zz = xor(z, s)
        block = dirs[pl.ds(zz * nb, nb)].reshape(zr, cols)
        facc[...] += jnp.dot(back[zz], block, preferred_element_type=f32)

    def finished(k):
        place = pl.ds(pl.multiple_of(k * own_rows, own_rows), own_rows)
        value, signs = facc[place, :], sgn_col[place, :]
        return jnp.concatenate(
            [value[:, j : j + 128] * signs for j in range(0, cols, 128)], axis=1
        ).astype(bf16)

    f_send[...] = finished(oc)
    f_copy = remote(f_send, f_recv, core_sems.at[0, 5], core_sems.at[1, 5], other)
    f_copy.start()
    full_ref[pl.ds(c, 1)] = finished(c)[None]

    for copy in (g_copy, f_copy):
        copy.wait_recv()
    ig_ref[pl.ds(oc, 1)] = g_recv[...][None]
    full_ref[pl.ds(oc, 1)] = f_recv[...][None]

    for p in range(4):
        tok_copy(p).wait_send()
    for copy in early + res_copies + [f_copy, g_copy]:
        copy.wait_send()
    for s in range(1, n_t):
        for k in range(2):
            hx_copy(s, k).wait_send()
        hf_copy(s).wait_send()
        for k in range(2 * nb):
            wx_copy(s, k).wait_send()
        for p in range(2):
            wz_copy(s, p).wait_send()
            for dy in y_peers:
                wy_copy(s, p, dy).wait_send()

    def sent(i, carry):
        for dy in y_peers:
            y_copy(i, dy).wait_send()
        for s in tensor_peers:
            x_copy(i, s).wait_send()
        return carry

    lax.fori_loop(0, nz, sent, 0)
    for i in range(nz - 1):
        z_copy(i).wait_send()
    for s in range(nz):
        for dy in range(nb):
            if s or dy:
                ag_copy(s, dy).wait_send()


def write_kernel(ig, nf, ns, full, ig_out, nf_out, ns_out, full_out, sems):
    half = ig.shape[2]
    copies = [(ig.at[k], ig_out.at[:, k * half : (k + 1) * half]) for k in range(2)]
    copies += [(full, full_out), (nf, nf_out), (ns, ns_out)]
    copies = [pltpu.make_async_copy(a, b, sems.at[i]) for i, (a, b) in enumerate(copies)]
    for copy in copies:
        copy.start()
    for copy in copies:
        copy.wait()


def shards(
    tokens, projection_weights, head_cotangent, frequencies, sign_bits, first_moment, second_moment
):
    rows, lw = tokens.shape
    n_t, n_dp = lax.axis_size("tensor"), lax.axis_size("dp")
    width = lw * n_t
    rank = frequencies.shape[1]
    own, cols = first_moment.shape[1], first_moment.shape[2]
    own_rows = projection_weights.shape[1] // n_dp
    chips = n_dp // 2
    cr = 2 * own
    nb = 2
    while nb * cr % 128:
        nb *= 2
    nz = chips // nb
    zr = nb * cr
    low_rows = min(128, 2 * own_rows)
    up8 = lambda n: -(-n // 8) * 8
    half = lw // 2

    anywhere, vmem = pl.BlockSpec(memory_space=pltpu.HBM), pl.BlockSpec(memory_space=pltpu.VMEM)
    dma = pltpu.SemaphoreType.DMA
    V = pltpu.VMEM
    args = (tokens, projection_weights, head_cotangent, frequencies, sign_bits, first_moment, second_moment)
    plan = (n_t, nz, nb, low_rows, rows * n_dp, width)
    ig, nf, ns, full = pl.pallas_call(
        functools.partial(main_kernel, plan),
        out_shape=(
            jax.ShapeDtypeStruct((2, rows, half), bf16),
            jax.ShapeDtypeStruct((2, own, cols), f32),
            jax.ShapeDtypeStruct((2, own, cols), f32),
            jax.ShapeDtypeStruct((2, own_rows, cols), bf16),
        ),
        in_specs=[anywhere] * 7,
        out_specs=(vmem,) * 4,
        scratch_shapes=[
            V((2, rows, lw), bf16), V((2, rows, lw), bf16), V((2, rank), jnp.int32),
            V((2, lw), jnp.int32), V((2, 2 * own_rows), jnp.int32),
            V((nz, low_rows, zr), f32), V((nz, low_rows, zr), f32),
            V((nz, up8(lw // low_rows), zr), f32), V((nz, up8(lw // low_rows), zr), f32),
            V((nz, up8(2 * own_rows // low_rows), zr), f32), V((nz, up8(2 * own_rows // low_rows), zr), f32),
            V((nz, 2 * own_rows, zr), bf16), V((2 * own_rows, 128), f32),
            V((n_t, 2, 2, rows, cols), bf16), V((2 * rows, n_t * cols), bf16), V((n_t, 2 * rows, 2 * cols), bf16),
            V((nz, nb, cr, n_t * cols), bf16), V((nz, nb - 1, cr, n_t * cols), bf16),
            V((nz, n_t, cr, cols), bf16), V((nz, n_t - 1, cr, cols), bf16),
            V((nz, cr, cols), bf16), V((nz, cr, cols), bf16),
            V((2, 2, own, cols), f32), V((2, 2, own, cols), f32), V((2, own, cols), f32),
            V((nz * nb, cr, cols), bf16), V((2 * own_rows, cols), f32),
            V((own_rows, cols), bf16), V((own_rows, cols), bf16),
            V((2, half, cols), bf16), V((n_t - 1, 2, half, cols), bf16),
            V((2 * rows, half), f32), V((rows, half), bf16), V((rows, half), bf16),
            dma((8,)), dma((2, 7)), dma((2, 4)), dma((2, n_t - 1, 2)), dma((2, n_t - 1)),
            dma((2, n_t - 1, 2 * nb)), dma((2, n_t - 1, 2, nb - 1)), dma((2, n_t - 1, 2)),
            dma((2, nz, nb - 1)), dma((2, nz, n_t - 1)), dma((2, nz)), dma((2, nz, nb)),
        ],
        compiler_params=pltpu.CompilerParams(
            collective_id=0, has_side_effects=True, vmem_limit_bytes=48 * 1024 * 1024
        ),
    )(*(pltpu.with_memory_space_constraint(a, pltpu.HBM) for a in args))
    return pl.pallas_call(
        write_kernel,
        out_shape=(
            jax.ShapeDtypeStruct((rows, lw), bf16),
            jax.ShapeDtypeStruct((2, own, cols), f32),
            jax.ShapeDtypeStruct((2, own, cols), f32),
            jax.ShapeDtypeStruct((2, own_rows, cols), bf16),
        ),
        in_specs=[vmem] * 4,
        out_specs=(anywhere,) * 4,
        scratch_shapes=[dma((5,))],
        compiler_params=pltpu.CompilerParams(vmem_limit_bytes=8 * 1024 * 1024),
    )(ig, nf, ns, full)


def solution(mesh):
    in_specs = (
        P("dp", "tensor"),
        P(None, None, "tensor"),
        P(None, "dp", "tensor"),
        P(),
        P(),
        P(None, "dp", "tensor"),
        P(None, "dp", "tensor"),
    )
    out_specs = (
        P("dp", "tensor"),
        P(None, "dp", "tensor"),
        P(None, "dp", "tensor"),
        P(None, "dp", "tensor"),
    )
    return jax.shard_map(shards, mesh=mesh, in_specs=in_specs, out_specs=out_specs, check_vma=False)
```

```python
import functools
import math

import jax
import jax.numpy as jnp
from jax import lax
from jax.experimental import pallas as pl
from jax.experimental.pallas import tpu as pltpu
from jax.sharding import PartitionSpec as P

first_fix = 1.0 - 0.9**10
second_fix = 1.0 - 0.95**10
epsilon = 1e-08
bf16, f32 = jnp.bfloat16, jnp.float32
RELAY0 = 2
DIRECT = 4


def wrap(value, period):
    return value & (period - 1) if period & (period - 1) == 0 else lax.rem(value, period)


def trig(phase, width):
    phase = wrap(phase, 4 * width)
    shift = width.bit_length() - 1
    quarter = (phase + width // 2) >> shift if 1 << shift == width else lax.div(phase + width // 2, width)
    x = (phase - quarter * width).astype(f32) * (math.pi / (2 * width))
    y = x * x
    c = 1.0 + y * (-0.5 + y * (1 / 24 + y * (-1 / 720 + y * (1 / 40320 - y * (1 / 3628800)))))
    s = x * (1.0 + y * (-1 / 6 + y * (1 / 120 + y * (-1 / 5040 + y * (1 / 362880)))))
    quarter = quarter & 3
    odd = (quarter & 1) == 1
    cosine = jnp.where(odd, s, c) * jnp.where((quarter == 1) | (quarter == 2), -1.0, 1.0)
    sine = jnp.where(odd, c, s) * jnp.where(quarter >= 2, -1.0, 1.0)
    return cosine, sine


def dot_last(a, b):
    return lax.dot_general(a, b, (((1,), (1,)), ((), ())), preferred_element_type=f32)


def main_kernel(
    plan,
    tok_ref, w_ref, hc_ref, freq_ref, sign_ref, first_ref, second_ref,
    ig_ref, nf_ref, ns_ref, full_ref,
    tok_all, tok_s, freq, sgn, sgn_b, cb, sb, ca, sa, ra, rb, back, sgn_col,
    hc_all, heads, pair_heads, y_send, y_recv, x_send, x_recv, d_recv, z_send, z_recv, mom, res, res_in, dirs, facc,
    f_send, f_recv, w_own, wp, g_acc, g_send, g_recv,
    loc, core_sems, g_sems, tok_sems, hx_sems, hf_sems, wx_sems, wy_sems, wz_sems, y_sems, x_sems, d_sems, z_sems, ag_sems,
):
    n_t, nz, nb, low_rows, token_count, width = plan
    rows, lw = tok_all.shape[1], tok_all.shape[2]
    rank = freq.shape[1]
    cr, cols = dirs.shape[1], dirs.shape[2]
    own = cr // 2
    zr = nb * cr
    own_rows = f_send.shape[0]
    half = lw // 2
    part = half // (2 * nb)
    piece = part // 2
    wide = min(512, half)
    deep = min(2048, lw)
    first_direct = max(0, nz - DIRECT)
    me_t, me_d = lax.axis_index("tensor"), lax.axis_index("dp")
    c, q = me_d % 2, me_d // 2
    y, z = q % nb, q // nb
    oc = 1 - c

    def dev(t, zz, yy, cc):
        return {"tensor": t, "dp": (zz * nb + yy) * 2 + cc}

    other = dev(me_t, z, y, oc)

    def xor(a, b):
        total, bit = 0, 1
        while bit < nz:
            total = total + bit * ((a // bit + b // bit) % 2)
            bit *= 2
        return total

    def remote(src, dst, send, recv, device):
        return pltpu.make_async_remote_copy(
            src_ref=src, dst_ref=dst, send_sem=send, recv_sem=recv,
            device_id=device, device_id_type=pl.DeviceIdType.MESH,
        )

    loads = [
        (freq_ref, freq),
        (tok_ref, tok_all.at[c]),
        (sign_ref.at[:, pl.ds(pl.multiple_of(me_t * lw, 128), lw)], sgn),
        (hc_ref, hc_all.at[me_t, c]),
        (sign_ref.at[:, pl.ds(pl.multiple_of(q * 2 * own_rows, 128), 2 * own_rows)], sgn_b),
        (first_ref.at[c], mom.at[0, c]),
        (second_ref.at[c], mom.at[1, c]),
        (w_ref.at[:, pl.ds(pl.multiple_of(me_t * lw + c * half, 128), half), :], w_own),
    ]
    loads = [pltpu.make_async_copy(a, b, loc.at[i]) for i, (a, b) in enumerate(loads)]
    for copy in loads:
        copy.start()

    barrier = pltpu.get_barrier_semaphore()
    peers = [other]
    for dy in range(1, nb):
        peers.append(dev(me_t, z, (y + dy) % nb, c))
    for dt in range(1, n_t):
        peers += [dev((me_t + dt) % n_t, z, y, c), dev((me_t + dt) % n_t, z, y, oc)]
        peers += [dev((me_t + dt) % n_t, z, (y + dy) % nb, c) for dy in range(1, nb)]
    for s in range(1, nz):
        peers.append(dev(me_t, xor(z, s), y, c))
    for device in peers:
        pl.semaphore_signal(barrier, inc=1, device_id=device, device_id_type=pl.DeviceIdType.MESH)

    loads[0].wait()
    f = jnp.where(c == 0, freq[0:1, :], freq[1:2, :])
    scale = jnp.where(f == 0, math.sqrt(1.0 / width), math.sqrt(2.0 / width)).astype(f32)

    def fill(cos_ref, sin_ref, start, stride, scaled):
        def block(r, carry):
            index = r * 8 + lax.broadcasted_iota(jnp.int32, (8, rank), 0)
            cosine, sine = trig((start + stride * index) * f, width)
            if scaled:
                cosine, sine = cosine * scale, sine * scale
            place = pl.ds(pl.multiple_of(r * 8, 8), 8)
            for k in range(nz):
                cos_ref[k, place, :] = cosine[:, k * zr : (k + 1) * zr]
                sin_ref[k, place, :] = sine[:, k * zr : (k + 1) * zr]
            return carry

        lax.fori_loop(0, cos_ref.shape[1] // 8, block, 0)

    fill(cb, sb, 1, 2, False)
    pl.semaphore_wait(barrier, len(peers))

    early = [
        remote(hc_ref, hc_all.at[me_t, c], core_sems.at[0, 0], core_sems.at[1, 0], other),
        remote(first_ref.at[oc], mom.at[0, c], core_sems.at[0, 1], core_sems.at[1, 1], other),
        remote(second_ref.at[oc], mom.at[1, c], core_sems.at[0, 2], core_sems.at[1, 2], other),
    ]

    def tensor_peer(s):
        return dev((me_t + s) % n_t, z, y, c)

    def hx_copy(s, k):
        m = (c + k) % 2
        return remote(
            hc_ref.at[m], hc_all.at[me_t, c, m], hx_sems.at[0, s - 1, k], hx_sems.at[1, s - 1, k],
            dev((me_t + s) % n_t, z, y, m),
        )

    def hf_copy(s):
        slot = hc_all.at[(me_t + n_t - s) % n_t, :, c]
        return remote(slot, slot, hf_sems.at[0, s - 1], hf_sems.at[1, s - 1], other)

    def tok_copy(p):
        place = slice(p * (lw // 4), (p + 1) * (lw // 4))
        return remote(
            tok_ref.at[:, place], tok_all.at[c, :, place], tok_sems.at[0, p], tok_sems.at[1, p], other
        )

    def rows_of(yy, zl, p):
        return pl.multiple_of((yy * 2 + zl) * part + p * piece, 16)

    zl = z % 2

    def wx_copy(s, k):
        yy, zz = (y, zl) if k < 2 else ((y + k // 2) % nb, 1 - zl)
        row = rows_of(yy, zz, k % 2)
        at = pl.ds(pl.multiple_of(((me_t + s) % n_t) * lw + c * half + row, 16), piece)
        return remote(
            w_ref.at[:, at, :], wp.at[s - 1, :, pl.ds(row, piece), :],
            wx_sems.at[0, s - 1, k], wx_sems.at[1, s - 1, k], tensor_peer(s),
        )

    def wy_copy(s, p, dy):
        slot = wp.at[s - 1, :, pl.ds(rows_of(y, zl, p), piece), :]
        return remote(
            slot, slot, wy_sems.at[0, s - 1, p, dy - 1], wy_sems.at[1, s - 1, p, dy - 1],
            dev(me_t, z, (y + dy) % nb, c),
        )

    def wz_copy(s, p):
        slot = wp.at[s - 1, :, pl.ds(rows_of(y, zl, p), piece), :]
        return remote(
            slot, slot, wz_sems.at[0, s - 1, p], wz_sems.at[1, s - 1, p], dev(me_t, xor(z, 1), y, c)
        )

    tensor_peers, y_peers = range(1, n_t), range(1, nb)

    def fetch(k):
        for s in tensor_peers:
            wx_copy(s, k).start()

    def relay_z(p):
        for s in tensor_peers:
            wx_copy(s, p).wait_recv()
            wz_copy(s, p).start()

    def relay_y(p):
        for s in tensor_peers:
            for dy in y_peers:
                wy_copy(s, p, dy).start()

    for s in range(1, n_t):
        for k in range(2):
            hx_copy(s, k).start()
    for p in range(4):
        tok_copy(p).start()
    for copy in early:
        copy.start()
    fetch(0)

    fill(ca, sa, 2 * me_t * lw, 2 * low_rows, True)

    def sign_tokens(k, start, count):
        for j in range(start, start + count, count // 2):
            place = slice(j, j + count // 2)
            row = jnp.where(c == 0, sgn[0:1, place], sgn[1:2, place])
            row = (2 * row - 1).astype(f32).astype(bf16)
            tok_s[pl.ds(k, 1), :, place] = tok_all[pl.ds(k, 1), :, place] * row

    loads[1].wait()
    loads[2].wait()
    for p in range(4):
        sign_tokens(c, p * (lw // 4), lw // 4)

    def tables(a_ref, b_ref, h, k):
        row = pl.ds(h, 1)
        return (a_ref[k, row, :] * cb[k] - b_ref[k, row, :] * sb[k]).astype(bf16)

    def y_copy(i, dy):
        yy = (y + dy) % nb
        return remote(
            y_send.at[i, yy], y_recv.at[i, dy - 1], y_sems.at[0, i, dy - 1], y_sems.at[1, i, dy - 1],
            dev(me_t, z, yy, c),
        )

    def x_copy(i, s):
        return remote(
            x_send.at[i, (me_t + s) % n_t], x_recv.at[i, s - 1],
            x_sems.at[0, i, s - 1], x_sems.at[1, i, s - 1], tensor_peer(s),
        )

    def z_copy(i):
        return remote(
            z_send.at[i], z_recv.at[i], z_sems.at[0, i], z_sems.at[1, i], dev(me_t, xor(z, nz - 1 - i), y, c)
        )

    corners = [(dt, dy) for dt in range(n_t) for dy in range(nb) if dt or dy]

    def corner_copy(i, dt, dy):
        t, yy, slot = (me_t + dt) % n_t, (y + dy) % nb, dt * nb + dy - 1
        return remote(
            y_send.at[i, yy, :, pl.ds(pl.multiple_of(t * cols, 128), cols)], d_recv.at[i - first_direct, slot],
            d_sems.at[0, i - first_direct, slot], d_sems.at[1, i - first_direct, slot], dev(t, z, yy, c),
        )

    def direct_sum(i):
        total = y_send[i, y, :, pl.ds(pl.multiple_of(me_t * cols, 128), cols)].astype(f32)
        for dt, dy in corners:
            corner_copy(i, dt, dy).wait_recv()
            total = total + d_recv[i - first_direct, dt * nb + dy - 1].astype(f32)
        return total

    def over_y(i):
        total = y_send[i, y].astype(f32)
        for dy in y_peers:
            y_copy(i, dy).wait_recv()
            total = total + y_recv[i, dy - 1].astype(f32)
        total = total.astype(bf16)
        for t in range(n_t):
            x_send[i, t] = total[:, t * cols : (t + 1) * cols]
        for s in tensor_peers:
            x_copy(i, s).start()

    def over_x(i):
        total = x_send[i, me_t].astype(f32)
        for s in tensor_peers:
            x_copy(i, s).wait_recv()
            total = total + x_recv[i, s - 1].astype(f32)
        return total

    def project(k, step, ready):
        projected = 0.0
        for j in range(0, lw, step):
            ready(j)
            basis = jnp.concatenate([tables(ca, sa, (j + h) // low_rows, k) for h in range(0, step, low_rows)], axis=0)
            signed = tok_s[:, :, j : j + step].reshape(2 * rows, step)
            projected = projected + jnp.dot(signed, basis, preferred_element_type=f32)
        return projected.astype(bf16)

    def low_rank(i, projected, direct):
        low = lax.dot_general(
            projected, heads[...], (((0,), (0,)), ((), ())), preferred_element_type=f32
        ).astype(bf16)
        for yy in range(nb):
            y_send[i, yy] = low[yy * cr : (yy + 1) * cr, :]
        if direct:
            for dt, dy in sorted(corners, key=lambda at: at[0] * at[1] == 0):
                corner_copy(i, dt, dy).start()
        else:
            for dy in y_peers:
                y_copy(i, dy).start()

    def arrive(j):
        tok_copy(j // (lw // 4)).wait_recv()
        sign_tokens(oc, j, lw // 4)

    projected = project(xor(z, nz - 1), lw // 4, arrive)
    loads[3].wait()
    early[0].wait_recv()
    for s in tensor_peers:
        for k in range(2):
            hx_copy(s, k).wait_recv()
    for t in range(n_t):
        heads[:, t * cols : (t + 1) * cols] = hc_all[t, :, pl.ds(c, 1)].reshape(2 * rows, cols)
    low_rank(0, projected, first_direct == 0)
    for s in tensor_peers:
        hf_copy(s).start()

    def chunks(start, stop, direct):
        def chunk(i, carry):
            low_rank(i, project(xor(z, nz - 1 - i), deep, lambda j: None), direct)

            @pl.when(i == RELAY0)
            def _():
                relay_z(0)

            return carry

        lax.fori_loop(start, stop, chunk, 0)

    if first_direct > 1:
        chunks(1, first_direct, False)
    chunks(max(1, first_direct), nz, True)

    def back_rows(h, carry):
        place = pl.ds(pl.multiple_of(h * low_rows, low_rows), low_rows)
        for k in range(nz):
            back[k, place, :] = tables(ra, rb, h, k)
        return carry

    def fill_back():
        fill(ra, rb, 2 * q * 2 * own_rows, 2 * low_rows, True)
        for s in tensor_peers:
            hf_copy(s).wait_recv()
        for t in range(n_t):
            for m in range(2):
                pair_heads[t, :, m * cols : (m + 1) * cols] = hc_all[t, :, m].reshape(2 * rows, cols)

    def build_back():
        lax.fori_loop(0, back.shape[1] // low_rows, back_rows, 0)

    def column_signs():
        loads[4].wait()
        lane = min(128, 2 * own_rows)
        for b in range(2 * own_rows // lane):
            at = slice(b * lane, (b + 1) * lane)
            row = (2 * jnp.where(c == 0, sgn_b[0:1, at], sgn_b[1:2, at]) - 1).astype(f32)
            sgn_col[b * lane : (b + 1) * lane, :] = jnp.broadcast_to(row, (128, lane)).T

    def own_gradient(j, carry):
        place = pl.ds(pl.multiple_of(j * wide, wide), wide)
        w = jnp.concatenate([w_own[m, place, :] for m in range(2)], axis=1)
        g_acc[:, place] = dot_last(pair_heads[me_t], w)
        return carry

    fillers = {0: fill_back, 1: build_back, 2: column_signs}

    def to_z(i, total):
        z_send[i] = total.astype(bf16)
        z_copy(i).start()

    for i in range(nz - 1):
        if i < first_direct:
            over_y(i)
        if i in fillers:
            fillers[i]()
        if 0 < i <= first_direct:
            to_z(i - 1, over_x(i - 1))
        if i >= first_direct:
            to_z(i, direct_sum(i))
        if i == nz - 2:
            fetch(1)
    if first_direct == nz - 1:
        to_z(nz - 2, over_x(nz - 2))
    relay_y(0)
    loads[7].wait()
    lax.fori_loop(0, half // wide, own_gradient, 0)
    for i in (5, 6):
        loads[i].wait()
    for i in (1, 2):
        early[i].wait_recv()

    total = direct_sum(nz - 1)
    for k in range(2, 2 * nb):
        fetch(k)
    for i in range(nz - 1):
        z_copy(i).wait_recv()
        total = total + z_recv[i].astype(f32)
    gradient = (total / math.sqrt(token_count)).reshape(2, own, cols)
    new_first = 0.9 * mom[0] + 0.1 * gradient
    new_second = 0.95 * mom[1] + 0.05 * gradient * gradient
    direction = new_first / first_fix / (jnp.sqrt(new_second / second_fix) + epsilon)
    dirs[pl.ds(z * nb + y, 1)] = direction.astype(bf16).reshape(1, cr, cols)

    def ag_copy(s, dy):
        if dy == 0:
            slot = dirs.at[z * nb + y]
            return remote(slot, slot, ag_sems.at[0, s, 0], ag_sems.at[1, s, 0], dev(me_t, xor(z, s), y, c))
        slot = dirs.at[xor(z, s) * nb + y]
        return remote(
            slot, slot, ag_sems.at[0, s, dy], ag_sems.at[1, s, dy], dev(me_t, z, (y + dy) % nb, c)
        )

    for s in range(nz - 1, 0, -1):
        ag_copy(s, 0).start()
    for dy in range(1, nb):
        ag_copy(0, dy).start()
    res[0] = new_first
    res[1] = new_second
    res_copies = [
        remote(res.at[k, oc], res_in.at[k], core_sems.at[0, 3 + k], core_sems.at[1, 3 + k], other)
        for k in range(2)
    ]
    for copy in res_copies:
        copy.start()

    for s in range(1, nz):
        ag_copy(s, 0).wait_recv()
        for dy in range(1, nb):
            ag_copy(s, dy).start()
        if s == min(1, nz - 1):
            relay_z(1)
            relay_y(1)
    def g_copy(k, place):
        return remote(g_send.at[:, place], g_recv.at[:, place], g_sems.at[0, k], g_sems.at[1, k], other)

    def add_gradient(k, place):
        value = g_acc[:, place]
        for s in tensor_peers:
            w = jnp.concatenate([wp[s - 1, m, place, :] for m in range(2)], axis=1)
            value = value + dot_last(pair_heads[(me_t + n_t - s) % n_t], w)
        g_acc[:, place] = value
        g_send[:, place] = g_acc[pl.ds(pl.multiple_of(oc * rows, rows), rows), place].astype(bf16)
        mine = g_acc[pl.ds(pl.multiple_of(c * rows, rows), rows), place].astype(bf16)
        ig_ref[pl.ds(c, 1), :, place] = mine[None]
        g_copy(k, place).start()

    pieces = [(y, zl, 0), (y, 1 - zl, 0)] + [((y + nb - dy) % nb, zl, 0) for dy in y_peers]
    pieces += [(y, zl, 1), (y, 1 - zl, 1)] + [((y + nb - dy) % nb, zl, 1) for dy in y_peers]
    pieces += [((y + dy) % nb, 1 - zl, p) for dy in y_peers for p in range(2)]
    fine = piece % 128 == 0
    places = [pl.ds(pl.multiple_of(rows_of(*at), 128), piece) for at in pieces] if fine else [slice(0, half)]

    def early_pieces(p):
        for s in tensor_peers:
            wz_copy(s, p).wait_recv()
            for dy in y_peers:
                wy_copy(s, p, dy).wait_recv()
        if fine:
            for k in range(p * (nb + 1), (p + 1) * (nb + 1)):
                add_gradient(k, places[k])

    def late_pieces():
        for j in range(2 * nb - 2):
            for s in tensor_peers:
                wx_copy(s, 2 + j).wait_recv()
            if fine:
                add_gradient(2 * (nb + 1) + j, places[2 * (nb + 1) + j])
        if not fine:
            add_gradient(0, places[0])

    early_pieces(0)
    nf_ref[pl.ds(c, 1)] = res[0, pl.ds(c, 1)]
    ns_ref[pl.ds(c, 1)] = res[1, pl.ds(c, 1)]
    for copy in res_copies:
        copy.wait_recv()
    nf_ref[pl.ds(oc, 1)] = res_in[0][None]
    ns_ref[pl.ds(oc, 1)] = res_in[1][None]
    facc[...] = jnp.zeros_like(facc)
    for s in range(nz):
        for dy in range(1, nb):
            ag_copy(s, dy).wait_recv()
        zz = xor(z, s)
        block = dirs[pl.ds(zz * nb, nb)].reshape(zr, cols)
        facc[...] += jnp.dot(back[zz], block, preferred_element_type=f32)

    def finished(k):
        place = pl.ds(pl.multiple_of(k * own_rows, own_rows), own_rows)
        value, signs = facc[place, :], sgn_col[place, :]
        return jnp.concatenate(
            [value[:, j : j + 128] * signs for j in range(0, cols, 128)], axis=1
        ).astype(bf16)

    f_send[...] = finished(oc)
    f_copy = remote(f_send, f_recv, core_sems.at[0, 5], core_sems.at[1, 5], other)
    f_copy.start()
    full_ref[pl.ds(c, 1)] = finished(c)[None]
    early_pieces(1)
    late_pieces()

    f_copy.wait_recv()
    for k, place in enumerate(places):
        g_copy(k, place).wait_recv()
    ig_ref[pl.ds(oc, 1)] = g_recv[...][None]
    full_ref[pl.ds(oc, 1)] = f_recv[...][None]

    for p in range(4):
        tok_copy(p).wait_send()
    for k, place in enumerate(places):
        g_copy(k, place).wait_send()
    for copy in early + res_copies + [f_copy]:
        copy.wait_send()
    for s in range(1, n_t):
        for k in range(2):
            hx_copy(s, k).wait_send()
        hf_copy(s).wait_send()
        for k in range(2 * nb):
            wx_copy(s, k).wait_send()
        for p in range(2):
            wz_copy(s, p).wait_send()
            for dy in y_peers:
                wy_copy(s, p, dy).wait_send()

    def sent(i, carry):
        for dy in y_peers:
            y_copy(i, dy).wait_send()
        for s in tensor_peers:
            x_copy(i, s).wait_send()
        return carry

    def sent_direct(i, carry):
        for dt, dy in corners:
            corner_copy(i, dt, dy).wait_send()
        return carry

    if first_direct:
        lax.fori_loop(0, first_direct, sent, 0)
    lax.fori_loop(first_direct, nz, sent_direct, 0)
    for i in range(nz - 1):
        z_copy(i).wait_send()
    for s in range(nz):
        for dy in range(nb):
            if s or dy:
                ag_copy(s, dy).wait_send()


def write_kernel(ig, nf, ns, full, ig_out, nf_out, ns_out, full_out, sems):
    half = ig.shape[2]
    copies = [(ig.at[k], ig_out.at[:, k * half : (k + 1) * half]) for k in range(2)]
    copies += [(full, full_out), (nf, nf_out), (ns, ns_out)]
    copies = [pltpu.make_async_copy(a, b, sems.at[i]) for i, (a, b) in enumerate(copies)]
    for copy in copies:
        copy.start()
    for copy in copies:
        copy.wait()


def shards(
    tokens, projection_weights, head_cotangent, frequencies, sign_bits, first_moment, second_moment
):
    rows, lw = tokens.shape
    n_t, n_dp = lax.axis_size("tensor"), lax.axis_size("dp")
    width = lw * n_t
    rank = frequencies.shape[1]
    own, cols = first_moment.shape[1], first_moment.shape[2]
    own_rows = projection_weights.shape[1] // n_dp
    chips = n_dp // 2
    cr = 2 * own
    nb = 2
    while nb * cr % 128:
        nb *= 2
    nz = chips // nb
    zr = nb * cr
    low_rows = min(128, 2 * own_rows)
    up8 = lambda n: -(-n // 8) * 8
    half = lw // 2

    anywhere, vmem = pl.BlockSpec(memory_space=pltpu.HBM), pl.BlockSpec(memory_space=pltpu.VMEM)
    dma = pltpu.SemaphoreType.DMA
    V = pltpu.VMEM
    args = (tokens, projection_weights, head_cotangent, frequencies, sign_bits, first_moment, second_moment)
    plan = (n_t, nz, nb, low_rows, rows * n_dp, width)
    ig, nf, ns, full = pl.pallas_call(
        functools.partial(main_kernel, plan),
        out_shape=(
            jax.ShapeDtypeStruct((2, rows, half), bf16),
            jax.ShapeDtypeStruct((2, own, cols), f32),
            jax.ShapeDtypeStruct((2, own, cols), f32),
            jax.ShapeDtypeStruct((2, own_rows, cols), bf16),
        ),
        in_specs=[anywhere] * 7,
        out_specs=(vmem,) * 4,
        scratch_shapes=[
            V((2, rows, lw), bf16), V((2, rows, lw), bf16), V((2, rank), jnp.int32),
            V((2, lw), jnp.int32), V((2, 2 * own_rows), jnp.int32),
            V((nz, low_rows, zr), f32), V((nz, low_rows, zr), f32),
            V((nz, up8(lw // low_rows), zr), f32), V((nz, up8(lw // low_rows), zr), f32),
            V((nz, up8(2 * own_rows // low_rows), zr), f32), V((nz, up8(2 * own_rows // low_rows), zr), f32),
            V((nz, 2 * own_rows, zr), bf16), V((2 * own_rows, 128), f32),
            V((n_t, 2, 2, rows, cols), bf16), V((2 * rows, n_t * cols), bf16), V((n_t, 2 * rows, 2 * cols), bf16),
            V((nz, nb, cr, n_t * cols), bf16), V((nz, nb - 1, cr, n_t * cols), bf16),
            V((nz, n_t, cr, cols), bf16), V((nz, n_t - 1, cr, cols), bf16),
            V((min(DIRECT, nz), n_t * nb - 1, cr, cols), bf16),
            V((nz, cr, cols), bf16), V((nz, cr, cols), bf16),
            V((2, 2, own, cols), f32), V((2, 2, own, cols), f32), V((2, own, cols), f32),
            V((nz * nb, cr, cols), bf16), V((2 * own_rows, cols), f32),
            V((own_rows, cols), bf16), V((own_rows, cols), bf16),
            V((2, half, cols), bf16), V((n_t - 1, 2, half, cols), bf16),
            V((2 * rows, half), f32), V((rows, half), bf16), V((rows, half), bf16),
            dma((8,)), dma((2, 6)), dma((2, 4 * nb)), dma((2, 4)), dma((2, n_t - 1, 2)), dma((2, n_t - 1)),
            dma((2, n_t - 1, 2 * nb)), dma((2, n_t - 1, 2, nb - 1)), dma((2, n_t - 1, 2)),
            dma((2, nz, nb - 1)), dma((2, nz, n_t - 1)),
            dma((2, min(DIRECT, nz), n_t * nb - 1)), dma((2, nz)), dma((2, nz, nb)),
        ],
        compiler_params=pltpu.CompilerParams(
            collective_id=0, has_side_effects=True, vmem_limit_bytes=48 * 1024 * 1024
        ),
    )(*(pltpu.with_memory_space_constraint(a, pltpu.HBM) for a in args))
    return pl.pallas_call(
        write_kernel,
        out_shape=(
            jax.ShapeDtypeStruct((rows, lw), bf16),
            jax.ShapeDtypeStruct((2, own, cols), f32),
            jax.ShapeDtypeStruct((2, own, cols), f32),
            jax.ShapeDtypeStruct((2, own_rows, cols), bf16),
        ),
        in_specs=[vmem] * 4,
        out_specs=(anywhere,) * 4,
        scratch_shapes=[dma((5,))],
        compiler_params=pltpu.CompilerParams(vmem_limit_bytes=8 * 1024 * 1024),
    )(ig, nf, ns, full)


def solution(mesh):
    in_specs = (
        P("dp", "tensor"),
        P(None, None, "tensor"),
        P(None, "dp", "tensor"),
        P(),
        P(),
        P(None, "dp", "tensor"),
        P(None, "dp", "tensor"),
    )
    out_specs = (
        P("dp", "tensor"),
        P(None, "dp", "tensor"),
        P(None, "dp", "tensor"),
        P(None, "dp", "tensor"),
    )
    return jax.shard_map(shards, mesh=mesh, in_specs=in_specs, out_specs=out_specs, check_vma=False)
```

```python
import functools
import math

import jax
import jax.numpy as jnp
from jax import lax
from jax.experimental import pallas as pl
from jax.experimental.pallas import tpu as pltpu
from jax.sharding import PartitionSpec as P

first_fix = 1.0 - 0.9**10
second_fix = 1.0 - 0.95**10
epsilon = 1e-08
bf16, f32 = jnp.bfloat16, jnp.float32
RELAY0 = 2
DIRECT = 4


def wrap(value, period):
    return value & (period - 1) if period & (period - 1) == 0 else lax.rem(value, period)


def trig(phase, width):
    phase = wrap(phase, 4 * width)
    shift = width.bit_length() - 1
    quarter = (phase + width // 2) >> shift if 1 << shift == width else lax.div(phase + width // 2, width)
    x = (phase - quarter * width).astype(f32) * (math.pi / (2 * width))
    y = x * x
    c = 1.0 + y * (-0.5 + y * (1 / 24 + y * (-1 / 720 + y * (1 / 40320 - y * (1 / 3628800)))))
    s = x * (1.0 + y * (-1 / 6 + y * (1 / 120 + y * (-1 / 5040 + y * (1 / 362880)))))
    quarter = quarter & 3
    odd = (quarter & 1) == 1
    cosine = jnp.where(odd, s, c) * jnp.where((quarter == 1) | (quarter == 2), -1.0, 1.0)
    sine = jnp.where(odd, c, s) * jnp.where(quarter >= 2, -1.0, 1.0)
    return cosine, sine


def dot_last(a, b):
    return lax.dot_general(a, b, (((1,), (1,)), ((), ())), preferred_element_type=f32)


def main_kernel(
    plan,
    tok_ref, w_ref, hc_ref, freq_ref, sign_ref, first_ref, second_ref,
    ig_ref, nf_ref, ns_ref, full_ref,
    tok_all, tok_s, freq, sgn, sgn_b, cb, sb, ca, sa, ra, rb, back, sgn_col,
    hc_all, heads, pair_heads, y_send, y_recv, x_send, x_recv, d_recv, z_send, z_recv, mom, res, res_in, dirs, facc,
    f_send, f_recv, w_own, wp, g_acc, g_send, g_recv,
    loc, core_sems, g_sems, tok_sems, hx_sems, hf_sems, wx_sems, wy_sems, wz_sems, y_sems, x_sems, d_sems, z_sems, ag_sems,
):
    n_t, nz, nb, low_rows, token_count, width = plan
    rows, lw = tok_all.shape[1], tok_all.shape[2]
    rank = freq.shape[1]
    cr, cols = dirs.shape[1], dirs.shape[2]
    own = cr // 2
    zr = nb * cr
    own_rows = f_send.shape[0]
    half = lw // 2
    part = half // (2 * nb)
    piece = part // 2
    wide = min(512, half)
    deep = min(2048, lw)
    first_direct = max(0, nz - DIRECT)
    me_t, me_d = lax.axis_index("tensor"), lax.axis_index("dp")
    c, q = me_d % 2, me_d // 2
    y, z = q % nb, q // nb
    oc = 1 - c

    def dev(t, zz, yy, cc):
        return {"tensor": t, "dp": (zz * nb + yy) * 2 + cc}

    other = dev(me_t, z, y, oc)

    def xor(a, b):
        total, bit = 0, 1
        while bit < nz:
            total = total + bit * ((a // bit + b // bit) % 2)
            bit *= 2
        return total

    def remote(src, dst, send, recv, device):
        return pltpu.make_async_remote_copy(
            src_ref=src, dst_ref=dst, send_sem=send, recv_sem=recv,
            device_id=device, device_id_type=pl.DeviceIdType.MESH,
        )

    loads = [
        (freq_ref, freq),
        (tok_ref, tok_all.at[c]),
        (sign_ref.at[:, pl.ds(pl.multiple_of(me_t * lw, 128), lw)], sgn),
        (hc_ref, hc_all.at[me_t, c]),
        (sign_ref.at[:, pl.ds(pl.multiple_of(q * 2 * own_rows, 128), 2 * own_rows)], sgn_b),
        (first_ref.at[c], mom.at[0, c]),
        (second_ref.at[c], mom.at[1, c]),
        (w_ref.at[:, pl.ds(pl.multiple_of(me_t * lw + c * half, 128), half), :], w_own),
    ]
    loads = [pltpu.make_async_copy(a, b, loc.at[i]) for i, (a, b) in enumerate(loads)]
    for copy in loads:
        copy.start()

    barrier = pltpu.get_barrier_semaphore()
    peers = [other]
    for dy in range(1, nb):
        peers.append(dev(me_t, z, (y + dy) % nb, c))
    for dt in range(1, n_t):
        peers += [dev((me_t + dt) % n_t, z, y, c), dev((me_t + dt) % n_t, z, y, oc)]
        peers += [dev((me_t + dt) % n_t, z, (y + dy) % nb, c) for dy in range(1, nb)]
    for s in range(1, nz):
        peers.append(dev(me_t, xor(z, s), y, c))
    for device in peers:
        pl.semaphore_signal(barrier, inc=1, device_id=device, device_id_type=pl.DeviceIdType.MESH)

    loads[0].wait()
    f = jnp.where(c == 0, freq[0:1, :], freq[1:2, :])
    scale = jnp.where(f == 0, math.sqrt(1.0 / width), math.sqrt(2.0 / width)).astype(f32)

    def fill(cos_ref, sin_ref, start, stride, scaled):
        def block(r, carry):
            index = r * 8 + lax.broadcasted_iota(jnp.int32, (8, rank), 0)
            cosine, sine = trig((start + stride * index) * f, width)
            if scaled:
                cosine, sine = cosine * scale, sine * scale
            place = pl.ds(pl.multiple_of(r * 8, 8), 8)
            for k in range(nz):
                cos_ref[k, place, :] = cosine[:, k * zr : (k + 1) * zr]
                sin_ref[k, place, :] = sine[:, k * zr : (k + 1) * zr]
            return carry

        lax.fori_loop(0, cos_ref.shape[1] // 8, block, 0)

    fill(cb, sb, 1, 2, False)
    pl.semaphore_wait(barrier, len(peers))

    early = [
        remote(hc_ref, hc_all.at[me_t, c], core_sems.at[0, 0], core_sems.at[1, 0], other),
        remote(first_ref.at[oc], mom.at[0, c], core_sems.at[0, 1], core_sems.at[1, 1], other),
        remote(second_ref.at[oc], mom.at[1, c], core_sems.at[0, 2], core_sems.at[1, 2], other),
    ]

    def tensor_peer(s):
        return dev((me_t + s) % n_t, z, y, c)

    def hx_copy(s, k):
        m = (c + k) % 2
        return remote(
            hc_ref.at[m], hc_all.at[me_t, c, m], hx_sems.at[0, s - 1, k], hx_sems.at[1, s - 1, k],
            dev((me_t + s) % n_t, z, y, m),
        )

    def hf_copy(s):
        slot = hc_all.at[(me_t + n_t - s) % n_t, :, c]
        return remote(slot, slot, hf_sems.at[0, s - 1], hf_sems.at[1, s - 1], other)

    def tok_copy(p):
        place = slice(p * (lw // 4), (p + 1) * (lw // 4))
        return remote(
            tok_ref.at[:, place], tok_all.at[c, :, place], tok_sems.at[0, p], tok_sems.at[1, p], other
        )

    def rows_of(yy, zl, p):
        return pl.multiple_of((yy * 2 + zl) * part + p * piece, 16)

    zl = z % 2

    def wx_copy(s, k):
        yy, zz = (y, zl) if k < 2 else ((y + k // 2) % nb, 1 - zl)
        row = rows_of(yy, zz, k % 2)
        at = pl.ds(pl.multiple_of(((me_t + s) % n_t) * lw + c * half + row, 16), piece)
        return remote(
            w_ref.at[:, at, :], wp.at[s - 1, :, pl.ds(row, piece), :],
            wx_sems.at[0, s - 1, k], wx_sems.at[1, s - 1, k], tensor_peer(s),
        )

    def wy_copy(s, p, dy):
        slot = wp.at[s - 1, :, pl.ds(rows_of(y, zl, p), piece), :]
        return remote(
            slot, slot, wy_sems.at[0, s - 1, p, dy - 1], wy_sems.at[1, s - 1, p, dy - 1],
            dev(me_t, z, (y + dy) % nb, c),
        )

    def wz_copy(s, p):
        slot = wp.at[s - 1, :, pl.ds(rows_of(y, zl, p), piece), :]
        return remote(
            slot, slot, wz_sems.at[0, s - 1, p], wz_sems.at[1, s - 1, p], dev(me_t, xor(z, 1), y, c)
        )

    tensor_peers, y_peers = range(1, n_t), range(1, nb)

    def fetch(k):
        for s in tensor_peers:
            wx_copy(s, k).start()

    def relay_z(p):
        for s in tensor_peers:
            wx_copy(s, p).wait_recv()
            wz_copy(s, p).start()

    def relay_y(p):
        for s in tensor_peers:
            for dy in y_peers:
                wy_copy(s, p, dy).start()

    for s in range(1, n_t):
        for k in range(2):
            hx_copy(s, k).start()
    for p in range(4):
        tok_copy(p).start()
    for copy in early:
        copy.start()
    fetch(0)

    fill(ca, sa, 2 * me_t * lw, 2 * low_rows, True)

    def sign_tokens(k, start, count):
        for j in range(start, start + count, count // 2):
            place = slice(j, j + count // 2)
            row = jnp.where(c == 0, sgn[0:1, place], sgn[1:2, place])
            row = (2 * row - 1).astype(f32).astype(bf16)
            tok_s[pl.ds(k, 1), :, place] = tok_all[pl.ds(k, 1), :, place] * row

    loads[1].wait()
    loads[2].wait()
    for p in range(4):
        sign_tokens(c, p * (lw // 4), lw // 4)

    def tables(a_ref, b_ref, h, k):
        row = pl.ds(h, 1)
        return (a_ref[k, row, :] * cb[k] - b_ref[k, row, :] * sb[k]).astype(bf16)

    def y_copy(i, dy):
        yy = (y + dy) % nb
        return remote(
            y_send.at[i, yy], y_recv.at[i, dy - 1], y_sems.at[0, i, dy - 1], y_sems.at[1, i, dy - 1],
            dev(me_t, z, yy, c),
        )

    def x_copy(i, s):
        return remote(
            x_send.at[i, (me_t + s) % n_t], x_recv.at[i, s - 1],
            x_sems.at[0, i, s - 1], x_sems.at[1, i, s - 1], tensor_peer(s),
        )

    def z_copy(i):
        return remote(
            z_send.at[i], z_recv.at[i], z_sems.at[0, i], z_sems.at[1, i], dev(me_t, xor(z, nz - 1 - i), y, c)
        )

    corners = [(dt, dy) for dt in range(n_t) for dy in range(nb) if dt or dy]

    def corner_copy(i, dt, dy):
        t, yy, slot = (me_t + dt) % n_t, (y + dy) % nb, dt * nb + dy - 1
        return remote(
            y_send.at[i, yy, :, pl.ds(pl.multiple_of(t * cols, 128), cols)], d_recv.at[i - first_direct, slot],
            d_sems.at[0, i - first_direct, slot], d_sems.at[1, i - first_direct, slot], dev(t, z, yy, c),
        )

    def direct_sum(i):
        total = y_send[i, y, :, pl.ds(pl.multiple_of(me_t * cols, 128), cols)].astype(f32)
        for dt, dy in corners:
            corner_copy(i, dt, dy).wait_recv()
            total = total + d_recv[i - first_direct, dt * nb + dy - 1].astype(f32)
        return total

    def over_y(i):
        total = y_send[i, y].astype(f32)
        for dy in y_peers:
            y_copy(i, dy).wait_recv()
            total = total + y_recv[i, dy - 1].astype(f32)
        total = total.astype(bf16)
        for t in range(n_t):
            x_send[i, t] = total[:, t * cols : (t + 1) * cols]
        for s in tensor_peers:
            x_copy(i, s).start()

    def over_x(i):
        total = x_send[i, me_t].astype(f32)
        for s in tensor_peers:
            x_copy(i, s).wait_recv()
            total = total + x_recv[i, s - 1].astype(f32)
        return total

    def project(k, step, ready):
        projected = 0.0
        for j in range(0, lw, step):
            ready(j)
            basis = jnp.concatenate([tables(ca, sa, (j + h) // low_rows, k) for h in range(0, step, low_rows)], axis=0)
            signed = tok_s[:, :, j : j + step].reshape(2 * rows, step)
            projected = projected + jnp.dot(signed, basis, preferred_element_type=f32)
        return projected.astype(bf16)

    def low_rank(i, projected, direct):
        low = lax.dot_general(
            projected, heads[...], (((0,), (0,)), ((), ())), preferred_element_type=f32
        ).astype(bf16)
        for yy in range(nb):
            y_send[i, yy] = low[yy * cr : (yy + 1) * cr, :]
        if direct:
            for dt, dy in sorted(corners, key=lambda at: at[0] * at[1] == 0):
                corner_copy(i, dt, dy).start()
        else:
            for dy in y_peers:
                y_copy(i, dy).start()

    def arrive(j):
        tok_copy(j // (lw // 4)).wait_recv()
        sign_tokens(oc, j, lw // 4)

    projected = project(xor(z, nz - 1), lw // 4, arrive)
    loads[3].wait()
    early[0].wait_recv()
    for s in tensor_peers:
        for k in range(2):
            hx_copy(s, k).wait_recv()
    for t in range(n_t):
        heads[:, t * cols : (t + 1) * cols] = hc_all[t, :, pl.ds(c, 1)].reshape(2 * rows, cols)
    low_rank(0, projected, first_direct == 0)
    for s in tensor_peers:
        hf_copy(s).start()

    def chunks(start, stop, direct):
        def chunk(i, carry):
            low_rank(i, project(xor(z, nz - 1 - i), deep, lambda j: None), direct)

            @pl.when(i == RELAY0)
            def _():
                relay_z(0)

            return carry

        lax.fori_loop(start, stop, chunk, 0)

    if first_direct > 1:
        chunks(1, first_direct, False)
    chunks(max(1, first_direct), nz, True)

    def back_rows(h, carry):
        place = pl.ds(pl.multiple_of(h * low_rows, low_rows), low_rows)
        for k in range(nz):
            back[k, place, :] = tables(ra, rb, h, k)
        return carry

    def fill_back():
        fill(ra, rb, 2 * q * 2 * own_rows, 2 * low_rows, True)
        for s in tensor_peers:
            hf_copy(s).wait_recv()
        for t in range(n_t):
            for m in range(2):
                pair_heads[t, :, m * cols : (m + 1) * cols] = hc_all[t, :, m].reshape(2 * rows, cols)

    def build_back():
        lax.fori_loop(0, back.shape[1] // low_rows, back_rows, 0)

    def column_signs():
        loads[4].wait()
        lane = min(128, 2 * own_rows)
        for b in range(2 * own_rows // lane):
            at = slice(b * lane, (b + 1) * lane)
            row = (2 * jnp.where(c == 0, sgn_b[0:1, at], sgn_b[1:2, at]) - 1).astype(f32)
            sgn_col[b * lane : (b + 1) * lane, :] = jnp.broadcast_to(row, (128, lane)).T

    def own_gradient(j, carry):
        place = pl.ds(pl.multiple_of(j * wide, wide), wide)
        w = jnp.concatenate([w_own[m, place, :] for m in range(2)], axis=1)
        g_acc[:, place] = dot_last(pair_heads[me_t], w)
        return carry

    fetch(1)
    fillers = {0: fill_back, 1: build_back, 2: column_signs}

    def to_z(i, total):
        z_send[i] = total.astype(bf16)
        z_copy(i).start()

    for i in range(nz - 1):
        if i < first_direct:
            over_y(i)
        if i in fillers:
            fillers[i]()
        if 0 < i <= first_direct:
            to_z(i - 1, over_x(i - 1))
        if i >= first_direct:
            to_z(i, direct_sum(i))
    if first_direct == nz - 1:
        to_z(nz - 2, over_x(nz - 2))
    relay_y(0)
    loads[7].wait()
    lax.fori_loop(0, half // wide, own_gradient, 0)
    for i in (5, 6):
        loads[i].wait()
    for i in (1, 2):
        early[i].wait_recv()

    total = direct_sum(nz - 1)
    for k in range(2, 2 * nb):
        fetch(k)
    for i in range(nz - 1):
        z_copy(i).wait_recv()
        total = total + z_recv[i].astype(f32)
    gradient = (total / math.sqrt(token_count)).reshape(2, own, cols)
    new_first = 0.9 * mom[0] + 0.1 * gradient
    new_second = 0.95 * mom[1] + 0.05 * gradient * gradient
    direction = new_first / first_fix / (jnp.sqrt(new_second / second_fix) + epsilon)
    dirs[pl.ds(z * nb + y, 1)] = direction.astype(bf16).reshape(1, cr, cols)

    def ag_copy(s, dy):
        if dy == 0:
            slot = dirs.at[z * nb + y]
            return remote(slot, slot, ag_sems.at[0, s, 0], ag_sems.at[1, s, 0], dev(me_t, xor(z, s), y, c))
        slot = dirs.at[xor(z, s) * nb + y]
        return remote(
            slot, slot, ag_sems.at[0, s, dy], ag_sems.at[1, s, dy], dev(me_t, z, (y + dy) % nb, c)
        )

    for s in range(nz - 1, 0, -1):
        ag_copy(s, 0).start()
    for dy in range(1, nb):
        ag_copy(0, dy).start()
    res[0] = new_first
    res[1] = new_second
    res_copies = [
        remote(res.at[k, oc], res_in.at[k], core_sems.at[0, 3 + k], core_sems.at[1, 3 + k], other)
        for k in range(2)
    ]
    for copy in res_copies:
        copy.start()
    relay_z(1)
    relay_y(1)

    for s in range(1, nz):
        ag_copy(s, 0).wait_recv()
        for dy in range(1, nb):
            ag_copy(s, dy).start()
    def g_copy(k, place):
        return remote(g_send.at[:, place], g_recv.at[:, place], g_sems.at[0, k], g_sems.at[1, k], other)

    def add_gradient(k, place):
        value = g_acc[:, place]
        for s in tensor_peers:
            w = jnp.concatenate([wp[s - 1, m, place, :] for m in range(2)], axis=1)
            value = value + dot_last(pair_heads[(me_t + n_t - s) % n_t], w)
        g_acc[:, place] = value
        g_send[:, place] = g_acc[pl.ds(pl.multiple_of(oc * rows, rows), rows), place].astype(bf16)
        mine = g_acc[pl.ds(pl.multiple_of(c * rows, rows), rows), place].astype(bf16)
        ig_ref[pl.ds(c, 1), :, place] = mine[None]
        g_copy(k, place).start()

    pieces = [(y, zl, 0), (y, 1 - zl, 0)] + [((y + nb - dy) % nb, zl, 0) for dy in y_peers]
    pieces += [(y, zl, 1), (y, 1 - zl, 1)] + [((y + nb - dy) % nb, zl, 1) for dy in y_peers]
    pieces += [((y + dy) % nb, 1 - zl, p) for dy in y_peers for p in range(2)]
    fine = piece % 128 == 0
    places = [pl.ds(pl.multiple_of(rows_of(*at), 128), piece) for at in pieces] if fine else [slice(0, half)]

    def early_pieces(p):
        for s in tensor_peers:
            wz_copy(s, p).wait_recv()
            for dy in y_peers:
                wy_copy(s, p, dy).wait_recv()
        if fine:
            for k in range(p * (nb + 1), (p + 1) * (nb + 1)):
                add_gradient(k, places[k])

    def late_pieces():
        for j in range(2 * nb - 2):
            for s in tensor_peers:
                wx_copy(s, 2 + j).wait_recv()
            if fine:
                add_gradient(2 * (nb + 1) + j, places[2 * (nb + 1) + j])
        if not fine:
            add_gradient(0, places[0])

    early_pieces(0)
    nf_ref[pl.ds(c, 1)] = res[0, pl.ds(c, 1)]
    ns_ref[pl.ds(c, 1)] = res[1, pl.ds(c, 1)]
    for copy in res_copies:
        copy.wait_recv()
    nf_ref[pl.ds(oc, 1)] = res_in[0][None]
    ns_ref[pl.ds(oc, 1)] = res_in[1][None]
    early_pieces(1)
    facc[...] = jnp.zeros_like(facc)
    for s in range(nz):
        for dy in range(1, nb):
            ag_copy(s, dy).wait_recv()
        zz = xor(z, s)
        block = dirs[pl.ds(zz * nb, nb)].reshape(zr, cols)
        facc[...] += jnp.dot(back[zz], block, preferred_element_type=f32)

    def finished(k):
        place = pl.ds(pl.multiple_of(k * own_rows, own_rows), own_rows)
        value, signs = facc[place, :], sgn_col[place, :]
        return jnp.concatenate(
            [value[:, j : j + 128] * signs for j in range(0, cols, 128)], axis=1
        ).astype(bf16)

    f_send[...] = finished(oc)
    f_copy = remote(f_send, f_recv, core_sems.at[0, 5], core_sems.at[1, 5], other)
    f_copy.start()
    full_ref[pl.ds(c, 1)] = finished(c)[None]
    late_pieces()

    f_copy.wait_recv()
    for k, place in enumerate(places):
        g_copy(k, place).wait_recv()
    ig_ref[pl.ds(oc, 1)] = g_recv[...][None]
    full_ref[pl.ds(oc, 1)] = f_recv[...][None]

    for p in range(4):
        tok_copy(p).wait_send()
    for k, place in enumerate(places):
        g_copy(k, place).wait_send()
    for copy in early + res_copies + [f_copy]:
        copy.wait_send()
    for s in range(1, n_t):
        for k in range(2):
            hx_copy(s, k).wait_send()
        hf_copy(s).wait_send()
        for k in range(2 * nb):
            wx_copy(s, k).wait_send()
        for p in range(2):
            wz_copy(s, p).wait_send()
            for dy in y_peers:
                wy_copy(s, p, dy).wait_send()

    def sent(i, carry):
        for dy in y_peers:
            y_copy(i, dy).wait_send()
        for s in tensor_peers:
            x_copy(i, s).wait_send()
        return carry

    def sent_direct(i, carry):
        for dt, dy in corners:
            corner_copy(i, dt, dy).wait_send()
        return carry

    if first_direct:
        lax.fori_loop(0, first_direct, sent, 0)
    lax.fori_loop(first_direct, nz, sent_direct, 0)
    for i in range(nz - 1):
        z_copy(i).wait_send()
    for s in range(nz):
        for dy in range(nb):
            if s or dy:
                ag_copy(s, dy).wait_send()


def write_kernel(ig, nf, ns, full, ig_out, nf_out, ns_out, full_out, sems):
    half = ig.shape[2]
    copies = [(ig.at[k], ig_out.at[:, k * half : (k + 1) * half]) for k in range(2)]
    copies += [(full, full_out), (nf, nf_out), (ns, ns_out)]
    copies = [pltpu.make_async_copy(a, b, sems.at[i]) for i, (a, b) in enumerate(copies)]
    for copy in copies:
        copy.start()
    for copy in copies:
        copy.wait()


def shards(
    tokens, projection_weights, head_cotangent, frequencies, sign_bits, first_moment, second_moment
):
    rows, lw = tokens.shape
    n_t, n_dp = lax.axis_size("tensor"), lax.axis_size("dp")
    width = lw * n_t
    rank = frequencies.shape[1]
    own, cols = first_moment.shape[1], first_moment.shape[2]
    own_rows = projection_weights.shape[1] // n_dp
    chips = n_dp // 2
    cr = 2 * own
    nb = 2
    while nb * cr % 128:
        nb *= 2
    nz = chips // nb
    zr = nb * cr
    low_rows = min(128, 2 * own_rows)
    up8 = lambda n: -(-n // 8) * 8
    half = lw // 2

    anywhere, vmem = pl.BlockSpec(memory_space=pltpu.HBM), pl.BlockSpec(memory_space=pltpu.VMEM)
    dma = pltpu.SemaphoreType.DMA
    V = pltpu.VMEM
    args = (tokens, projection_weights, head_cotangent, frequencies, sign_bits, first_moment, second_moment)
    plan = (n_t, nz, nb, low_rows, rows * n_dp, width)
    ig, nf, ns, full = pl.pallas_call(
        functools.partial(main_kernel, plan),
        out_shape=(
            jax.ShapeDtypeStruct((2, rows, half), bf16),
            jax.ShapeDtypeStruct((2, own, cols), f32),
            jax.ShapeDtypeStruct((2, own, cols), f32),
            jax.ShapeDtypeStruct((2, own_rows, cols), bf16),
        ),
        in_specs=[anywhere] * 7,
        out_specs=(vmem,) * 4,
        scratch_shapes=[
            V((2, rows, lw), bf16), V((2, rows, lw), bf16), V((2, rank), jnp.int32),
            V((2, lw), jnp.int32), V((2, 2 * own_rows), jnp.int32),
            V((nz, low_rows, zr), f32), V((nz, low_rows, zr), f32),
            V((nz, up8(lw // low_rows), zr), f32), V((nz, up8(lw // low_rows), zr), f32),
            V((nz, up8(2 * own_rows // low_rows), zr), f32), V((nz, up8(2 * own_rows // low_rows), zr), f32),
            V((nz, 2 * own_rows, zr), bf16), V((2 * own_rows, 128), f32),
            V((n_t, 2, 2, rows, cols), bf16), V((2 * rows, n_t * cols), bf16), V((n_t, 2 * rows, 2 * cols), bf16),
            V((nz, nb, cr, n_t * cols), bf16), V((nz, nb - 1, cr, n_t * cols), bf16),
            V((nz, n_t, cr, cols), bf16), V((nz, n_t - 1, cr, cols), bf16),
            V((min(DIRECT, nz), n_t * nb - 1, cr, cols), bf16),
            V((nz, cr, cols), bf16), V((nz, cr, cols), bf16),
            V((2, 2, own, cols), f32), V((2, 2, own, cols), f32), V((2, own, cols), f32),
            V((nz * nb, cr, cols), bf16), V((2 * own_rows, cols), f32),
            V((own_rows, cols), bf16), V((own_rows, cols), bf16),
            V((2, half, cols), bf16), V((n_t - 1, 2, half, cols), bf16),
            V((2 * rows, half), f32), V((rows, half), bf16), V((rows, half), bf16),
            dma((8,)), dma((2, 6)), dma((2, 4 * nb)), dma((2, 4)), dma((2, n_t - 1, 2)), dma((2, n_t - 1)),
            dma((2, n_t - 1, 2 * nb)), dma((2, n_t - 1, 2, nb - 1)), dma((2, n_t - 1, 2)),
            dma((2, nz, nb - 1)), dma((2, nz, n_t - 1)),
            dma((2, min(DIRECT, nz), n_t * nb - 1)), dma((2, nz)), dma((2, nz, nb)),
        ],
        compiler_params=pltpu.CompilerParams(
            collective_id=0, has_side_effects=True, vmem_limit_bytes=48 * 1024 * 1024
        ),
    )(*(pltpu.with_memory_space_constraint(a, pltpu.HBM) for a in args))
    return pl.pallas_call(
        write_kernel,
        out_shape=(
            jax.ShapeDtypeStruct((rows, lw), bf16),
            jax.ShapeDtypeStruct((2, own, cols), f32),
            jax.ShapeDtypeStruct((2, own, cols), f32),
            jax.ShapeDtypeStruct((2, own_rows, cols), bf16),
        ),
        in_specs=[vmem] * 4,
        out_specs=(anywhere,) * 4,
        scratch_shapes=[dma((5,))],
        compiler_params=pltpu.CompilerParams(vmem_limit_bytes=8 * 1024 * 1024),
    )(ig, nf, ns, full)


def solution(mesh):
    in_specs = (
        P("dp", "tensor"),
        P(None, None, "tensor"),
        P(None, "dp", "tensor"),
        P(),
        P(),
        P(None, "dp", "tensor"),
        P(None, "dp", "tensor"),
    )
    out_specs = (
        P("dp", "tensor"),
        P(None, "dp", "tensor"),
        P(None, "dp", "tensor"),
        P(None, "dp", "tensor"),
    )
    return jax.shard_map(shards, mesh=mesh, in_specs=in_specs, out_specs=out_specs, check_vma=False)
```

```python
import functools
import math

import jax
import jax.numpy as jnp
from jax import lax
from jax.experimental import pallas as pl
from jax.experimental.pallas import tpu as pltpu
from jax.sharding import PartitionSpec as P

first_fix = 1.0 - 0.9**10
second_fix = 1.0 - 0.95**10
epsilon = 1e-08
bf16, f32 = jnp.bfloat16, jnp.float32
RELAY0 = 2
DIRECT = 4


def wrap(value, period):
    return value & (period - 1) if period & (period - 1) == 0 else lax.rem(value, period)


def trig(phase, width):
    phase = wrap(phase, 4 * width)
    shift = width.bit_length() - 1
    quarter = (phase + width // 2) >> shift if 1 << shift == width else lax.div(phase + width // 2, width)
    x = (phase - quarter * width).astype(f32) * (math.pi / (2 * width))
    y = x * x
    c = 1.0 + y * (-0.5 + y * (1 / 24 + y * (-1 / 720 + y * (1 / 40320 - y * (1 / 3628800)))))
    s = x * (1.0 + y * (-1 / 6 + y * (1 / 120 + y * (-1 / 5040 + y * (1 / 362880)))))
    quarter = quarter & 3
    odd = (quarter & 1) == 1
    cosine = jnp.where(odd, s, c) * jnp.where((quarter == 1) | (quarter == 2), -1.0, 1.0)
    sine = jnp.where(odd, c, s) * jnp.where(quarter >= 2, -1.0, 1.0)
    return cosine, sine


def dot_last(a, b):
    return lax.dot_general(a, b, (((1,), (1,)), ((), ())), preferred_element_type=f32)


def main_kernel(
    plan,
    tok_ref, w_ref, hc_ref, freq_ref, sign_ref, first_ref, second_ref,
    ig_ref, nf_ref, ns_ref, full_ref,
    tok_all, tok_s, freq, sgn, sgn_b, cb, sb, ca, sa, ra, rb, back, sgn_col,
    hc_all, heads, pair_heads, y_send, y_recv, x_send, x_recv, d_recv, z_send, z_recv, mom, res, res_in, dirs, facc,
    f_send, f_recv, w_own, wp, g_acc, g_send, g_recv,
    loc, core_sems, g_sems, tok_sems, hx_sems, hf_sems, wx_sems, wy_sems, wz_sems, y_sems, x_sems, d_sems, z_sems, ag_sems,
):
    n_t, nz, nb, low_rows, token_count, width = plan
    rows, lw = tok_all.shape[1], tok_all.shape[2]
    rank = freq.shape[1]
    cr, cols = dirs.shape[1], dirs.shape[2]
    own = cr // 2
    zr = nb * cr
    own_rows = f_send.shape[0]
    half = lw // 2
    part = half // (2 * nb)
    piece = part // 2
    wide = min(512, half)
    deep = min(2048, lw)
    first_direct = max(0, nz - DIRECT)
    me_t, me_d = lax.axis_index("tensor"), lax.axis_index("dp")
    c, q = me_d % 2, me_d // 2
    y, z = q % nb, q // nb
    oc = 1 - c

    def dev(t, zz, yy, cc):
        return {"tensor": t, "dp": (zz * nb + yy) * 2 + cc}

    other = dev(me_t, z, y, oc)

    def xor(a, b):
        total, bit = 0, 1
        while bit < nz:
            total = total + bit * ((a // bit + b // bit) % 2)
            bit *= 2
        return total

    def remote(src, dst, send, recv, device):
        return pltpu.make_async_remote_copy(
            src_ref=src, dst_ref=dst, send_sem=send, recv_sem=recv,
            device_id=device, device_id_type=pl.DeviceIdType.MESH,
        )

    loads = [
        (freq_ref, freq),
        (tok_ref, tok_all.at[c]),
        (sign_ref.at[:, pl.ds(pl.multiple_of(me_t * lw, 128), lw)], sgn),
        (hc_ref, hc_all.at[me_t, c]),
        (sign_ref.at[:, pl.ds(pl.multiple_of(q * 2 * own_rows, 128), 2 * own_rows)], sgn_b),
        (first_ref.at[c], mom.at[0, c]),
        (second_ref.at[c], mom.at[1, c]),
        (w_ref.at[:, pl.ds(pl.multiple_of(me_t * lw + c * half, 128), half), :], w_own),
    ]
    loads = [pltpu.make_async_copy(a, b, loc.at[i]) for i, (a, b) in enumerate(loads)]
    for copy in loads:
        copy.start()

    barrier = pltpu.get_barrier_semaphore()
    peers = [other]
    for dy in range(1, nb):
        peers.append(dev(me_t, z, (y + dy) % nb, c))
    for dt in range(1, n_t):
        peers += [dev((me_t + dt) % n_t, z, y, c), dev((me_t + dt) % n_t, z, y, oc)]
        peers += [dev((me_t + dt) % n_t, z, (y + dy) % nb, c) for dy in range(1, nb)]
    for s in range(1, nz):
        peers.append(dev(me_t, xor(z, s), y, c))
    for device in peers:
        pl.semaphore_signal(barrier, inc=1, device_id=device, device_id_type=pl.DeviceIdType.MESH)

    loads[0].wait()
    f = jnp.where(c == 0, freq[0:1, :], freq[1:2, :])
    scale = jnp.where(f == 0, math.sqrt(1.0 / width), math.sqrt(2.0 / width)).astype(f32)

    def fill(cos_ref, sin_ref, start, stride, scaled):
        def block(r, carry):
            index = r * 8 + lax.broadcasted_iota(jnp.int32, (8, rank), 0)
            cosine, sine = trig((start + stride * index) * f, width)
            if scaled:
                cosine, sine = cosine * scale, sine * scale
            place = pl.ds(pl.multiple_of(r * 8, 8), 8)
            for k in range(nz):
                cos_ref[k, place, :] = cosine[:, k * zr : (k + 1) * zr]
                sin_ref[k, place, :] = sine[:, k * zr : (k + 1) * zr]
            return carry

        lax.fori_loop(0, cos_ref.shape[1] // 8, block, 0)

    fill(cb, sb, 1, 2, False)
    pl.semaphore_wait(barrier, len(peers))

    early = [
        remote(hc_ref, hc_all.at[me_t, c], core_sems.at[0, 0], core_sems.at[1, 0], other),
        remote(first_ref.at[oc], mom.at[0, c], core_sems.at[0, 1], core_sems.at[1, 1], other),
        remote(second_ref.at[oc], mom.at[1, c], core_sems.at[0, 2], core_sems.at[1, 2], other),
    ]

    def tensor_peer(s):
        return dev((me_t + s) % n_t, z, y, c)

    def hx_copy(s, k):
        m = (c + k) % 2
        return remote(
            hc_ref.at[m], hc_all.at[me_t, c, m], hx_sems.at[0, s - 1, k], hx_sems.at[1, s - 1, k],
            dev((me_t + s) % n_t, z, y, m),
        )

    def hf_copy(s):
        slot = hc_all.at[(me_t + n_t - s) % n_t, :, c]
        return remote(slot, slot, hf_sems.at[0, s - 1], hf_sems.at[1, s - 1], other)

    def tok_copy(p):
        place = slice(p * (lw // 4), (p + 1) * (lw // 4))
        return remote(
            tok_ref.at[:, place], tok_all.at[c, :, place], tok_sems.at[0, p], tok_sems.at[1, p], other
        )

    def rows_of(yy, zl, p):
        return pl.multiple_of((yy * 2 + zl) * part + p * piece, 16)

    zl = z % 2

    def wx_copy(s, k):
        yy, zz = (y, zl) if k < 2 else ((y + k // 2) % nb, 1 - zl)
        row = rows_of(yy, zz, k % 2)
        at = pl.ds(pl.multiple_of(((me_t + s) % n_t) * lw + c * half + row, 16), piece)
        return remote(
            w_ref.at[:, at, :], wp.at[s - 1, :, pl.ds(row, piece), :],
            wx_sems.at[0, s - 1, k], wx_sems.at[1, s - 1, k], tensor_peer(s),
        )

    def wy_copy(s, p, dy):
        slot = wp.at[s - 1, :, pl.ds(rows_of(y, zl, p), piece), :]
        return remote(
            slot, slot, wy_sems.at[0, s - 1, p, dy - 1], wy_sems.at[1, s - 1, p, dy - 1],
            dev(me_t, z, (y + dy) % nb, c),
        )

    def wz_copy(s, p):
        slot = wp.at[s - 1, :, pl.ds(rows_of(y, zl, p), piece), :]
        return remote(
            slot, slot, wz_sems.at[0, s - 1, p], wz_sems.at[1, s - 1, p], dev(me_t, xor(z, 1), y, c)
        )

    tensor_peers, y_peers = range(1, n_t), range(1, nb)

    def fetch(k):
        for s in tensor_peers:
            wx_copy(s, k).start()

    def relay_z(p):
        for s in tensor_peers:
            wx_copy(s, p).wait_recv()
            wz_copy(s, p).start()

    def relay_y(p):
        for s in tensor_peers:
            for dy in y_peers:
                wy_copy(s, p, dy).start()

    for s in range(1, n_t):
        for k in range(2):
            hx_copy(s, k).start()
    for p in range(4):
        tok_copy(p).start()
    for copy in early:
        copy.start()
    fetch(0)

    fill(ca, sa, 2 * me_t * lw, 2 * low_rows, True)

    def sign_tokens(k, start, count):
        for j in range(start, start + count, count // 2):
            place = slice(j, j + count // 2)
            row = jnp.where(c == 0, sgn[0:1, place], sgn[1:2, place])
            row = (2 * row - 1).astype(f32).astype(bf16)
            tok_s[pl.ds(k, 1), :, place] = tok_all[pl.ds(k, 1), :, place] * row

    loads[1].wait()
    loads[2].wait()
    for p in range(4):
        sign_tokens(c, p * (lw // 4), lw // 4)

    def tables(a_ref, b_ref, h, k):
        row = pl.ds(h, 1)
        return (a_ref[k, row, :] * cb[k] - b_ref[k, row, :] * sb[k]).astype(bf16)

    def y_copy(i, dy):
        yy = (y + dy) % nb
        return remote(
            y_send.at[i, yy], y_recv.at[i, dy - 1], y_sems.at[0, i, dy - 1], y_sems.at[1, i, dy - 1],
            dev(me_t, z, yy, c),
        )

    def x_copy(i, s):
        return remote(
            x_send.at[i, (me_t + s) % n_t], x_recv.at[i, s - 1],
            x_sems.at[0, i, s - 1], x_sems.at[1, i, s - 1], tensor_peer(s),
        )

    def z_copy(i):
        return remote(
            z_send.at[i], z_recv.at[i], z_sems.at[0, i], z_sems.at[1, i], dev(me_t, xor(z, nz - 1 - i), y, c)
        )

    corners = [(dt, dy) for dt in range(n_t) for dy in range(nb) if dt or dy]

    def corner_copy(i, dt, dy):
        t, yy, slot = (me_t + dt) % n_t, (y + dy) % nb, dt * nb + dy - 1
        return remote(
            y_send.at[i, yy, :, pl.ds(pl.multiple_of(t * cols, 128), cols)], d_recv.at[i - first_direct, slot],
            d_sems.at[0, i - first_direct, slot], d_sems.at[1, i - first_direct, slot], dev(t, z, yy, c),
        )

    def direct_sum(i):
        total = y_send[i, y, :, pl.ds(pl.multiple_of(me_t * cols, 128), cols)].astype(f32)
        for dt, dy in corners:
            corner_copy(i, dt, dy).wait_recv()
            total = total + d_recv[i - first_direct, dt * nb + dy - 1].astype(f32)
        return total

    def over_y(i):
        total = y_send[i, y].astype(f32)
        for dy in y_peers:
            y_copy(i, dy).wait_recv()
            total = total + y_recv[i, dy - 1].astype(f32)
        total = total.astype(bf16)
        for t in range(n_t):
            x_send[i, t] = total[:, t * cols : (t + 1) * cols]
        for s in tensor_peers:
            x_copy(i, s).start()

    def over_x(i):
        total = x_send[i, me_t].astype(f32)
        for s in tensor_peers:
            x_copy(i, s).wait_recv()
            total = total + x_recv[i, s - 1].astype(f32)
        return total

    def project(k, step, ready):
        projected = 0.0
        for j in range(0, lw, step):
            ready(j)
            basis = jnp.concatenate([tables(ca, sa, (j + h) // low_rows, k) for h in range(0, step, low_rows)], axis=0)
            signed = tok_s[:, :, j : j + step].reshape(2 * rows, step)
            projected = projected + jnp.dot(signed, basis, preferred_element_type=f32)
        return projected.astype(bf16)

    def low_rank(i, projected, direct):
        low = lax.dot_general(
            projected, heads[...], (((0,), (0,)), ((), ())), preferred_element_type=f32
        ).astype(bf16)
        for yy in range(nb):
            y_send[i, yy] = low[yy * cr : (yy + 1) * cr, :]
        if direct:
            for dt, dy in sorted(corners, key=lambda at: at[0] * at[1] == 0):
                corner_copy(i, dt, dy).start()
        else:
            for dy in y_peers:
                y_copy(i, dy).start()

    def arrive(j):
        tok_copy(j // (lw // 4)).wait_recv()
        sign_tokens(oc, j, lw // 4)

    projected = project(xor(z, nz - 1), lw // 4, arrive)
    loads[3].wait()
    early[0].wait_recv()
    for s in tensor_peers:
        for k in range(2):
            hx_copy(s, k).wait_recv()
    for t in range(n_t):
        heads[:, t * cols : (t + 1) * cols] = hc_all[t, :, pl.ds(c, 1)].reshape(2 * rows, cols)
    low_rank(0, projected, first_direct == 0)
    for s in tensor_peers:
        hf_copy(s).start()

    def chunks(start, stop, direct):
        def chunk(i, carry):
            low_rank(i, project(xor(z, nz - 1 - i), deep, lambda j: None), direct)

            @pl.when(i == RELAY0)
            def _():
                relay_z(0)

            return carry

        lax.fori_loop(start, stop, chunk, 0)

    if first_direct > 1:
        chunks(1, first_direct, False)
    chunks(max(1, first_direct), nz, True)

    def back_rows(h, carry):
        place = pl.ds(pl.multiple_of(h * low_rows, low_rows), low_rows)
        for k in range(nz):
            back[k, place, :] = tables(ra, rb, h, k)
        return carry

    def fill_back():
        fill(ra, rb, 2 * q * 2 * own_rows, 2 * low_rows, True)
        for s in tensor_peers:
            hf_copy(s).wait_recv()
        for t in range(n_t):
            for m in range(2):
                pair_heads[t, :, m * cols : (m + 1) * cols] = hc_all[t, :, m].reshape(2 * rows, cols)

    def build_back():
        lax.fori_loop(0, back.shape[1] // low_rows, back_rows, 0)

    def column_signs():
        loads[4].wait()
        lane = min(128, 2 * own_rows)
        for b in range(2 * own_rows // lane):
            at = slice(b * lane, (b + 1) * lane)
            row = (2 * jnp.where(c == 0, sgn_b[0:1, at], sgn_b[1:2, at]) - 1).astype(f32)
            sgn_col[b * lane : (b + 1) * lane, :] = jnp.broadcast_to(row, (128, lane)).T

    def own_gradient(j, carry):
        place = pl.ds(pl.multiple_of(j * wide, wide), wide)
        w = jnp.concatenate([w_own[m, place, :] for m in range(2)], axis=1)
        g_acc[:, place] = dot_last(pair_heads[me_t], w)
        return carry

    fetch(1)
    fillers = {0: fill_back, 1: build_back, 2: column_signs}

    def to_z(i, total):
        z_send[i] = total.astype(bf16)
        z_copy(i).start()

    for i in range(nz - 1):
        if i < first_direct:
            over_y(i)
        if i in fillers:
            fillers[i]()
        if 0 < i <= first_direct:
            to_z(i - 1, over_x(i - 1))
        if i >= first_direct:
            to_z(i, direct_sum(i))
    if first_direct == nz - 1:
        to_z(nz - 2, over_x(nz - 2))
    relay_y(0)
    loads[7].wait()
    lax.fori_loop(0, half // wide, own_gradient, 0)
    for i in (5, 6):
        loads[i].wait()
    for i in (1, 2):
        early[i].wait_recv()

    total = direct_sum(nz - 1)
    for k in range(2, 2 * nb):
        fetch(k)
    for i in range(nz - 1):
        z_copy(i).wait_recv()
        total = total + z_recv[i].astype(f32)
    gradient = (total / math.sqrt(token_count)).reshape(2, own, cols)
    new_first = 0.9 * mom[0] + 0.1 * gradient
    new_second = 0.95 * mom[1] + 0.05 * gradient * gradient
    direction = new_first / first_fix / (jnp.sqrt(new_second / second_fix) + epsilon)
    dirs[pl.ds(z * nb + y, 1)] = direction.astype(bf16).reshape(1, cr, cols)

    def ag_copy(s, dy):
        if dy == 0:
            slot = dirs.at[z * nb + y]
            return remote(slot, slot, ag_sems.at[0, s, 0], ag_sems.at[1, s, 0], dev(me_t, xor(z, s), y, c))
        slot = dirs.at[xor(z, s) * nb + y]
        return remote(
            slot, slot, ag_sems.at[0, s, dy], ag_sems.at[1, s, dy], dev(me_t, z, (y + dy) % nb, c)
        )

    for s in range(nz - 1, 0, -1):
        ag_copy(s, 0).start()
    for dy in range(1, nb):
        ag_copy(0, dy).start()
    res[0] = new_first
    res[1] = new_second
    res_copies = [
        remote(res.at[k, oc], res_in.at[k], core_sems.at[0, 3 + k], core_sems.at[1, 3 + k], other)
        for k in range(2)
    ]
    for copy in res_copies:
        copy.start()
    relay_z(1)
    relay_y(1)

    for s in range(1, nz):
        ag_copy(s, 0).wait_recv()
        for dy in range(1, nb):
            ag_copy(s, dy).start()
    def g_copy(k, place):
        return remote(g_send.at[:, place], g_recv.at[:, place], g_sems.at[0, k], g_sems.at[1, k], other)

    def add_gradient(k, place):
        value = g_acc[:, place]
        for s in tensor_peers:
            w = jnp.concatenate([wp[s - 1, m, place, :] for m in range(2)], axis=1)
            value = value + dot_last(pair_heads[(me_t + n_t - s) % n_t], w)
        g_acc[:, place] = value
        g_send[:, place] = g_acc[pl.ds(pl.multiple_of(oc * rows, rows), rows), place].astype(bf16)
        mine = g_acc[pl.ds(pl.multiple_of(c * rows, rows), rows), place].astype(bf16)
        ig_ref[pl.ds(c, 1), :, place] = mine[None]
        g_copy(k, place).start()

    pieces = [(y, zl, 0), (y, 1 - zl, 0)] + [((y + nb - dy) % nb, zl, 0) for dy in y_peers]
    pieces += [(y, zl, 1), (y, 1 - zl, 1)] + [((y + nb - dy) % nb, zl, 1) for dy in y_peers]
    pieces += [((y + dy) % nb, 1 - zl, p) for dy in y_peers for p in range(2)]
    fine = piece % 128 == 0
    places = [pl.ds(pl.multiple_of(rows_of(*at), 128), piece) for at in pieces] if fine else [slice(0, half)]

    def early_pieces(p):
        for s in tensor_peers:
            wz_copy(s, p).wait_recv()
            for dy in y_peers:
                wy_copy(s, p, dy).wait_recv()
        if fine:
            for k in range(p * (nb + 1), (p + 1) * (nb + 1)):
                add_gradient(k, places[k])

    def late_pieces():
        for j in range(2 * nb - 2):
            for s in tensor_peers:
                wx_copy(s, 2 + j).wait_recv()
            if fine:
                add_gradient(2 * (nb + 1) + j, places[2 * (nb + 1) + j])
        if not fine:
            add_gradient(0, places[0])

    early_pieces(0)
    nf_ref[pl.ds(c, 1)] = res[0, pl.ds(c, 1)]
    ns_ref[pl.ds(c, 1)] = res[1, pl.ds(c, 1)]
    for copy in res_copies:
        copy.wait_recv()
    nf_ref[pl.ds(oc, 1)] = res_in[0][None]
    ns_ref[pl.ds(oc, 1)] = res_in[1][None]
    early_pieces(1)
    facc[...] = jnp.zeros_like(facc)
    for s in range(nz):
        for dy in range(1, nb):
            ag_copy(s, dy).wait_recv()
        zz = xor(z, s)
        block = dirs[pl.ds(zz * nb, nb)].reshape(zr, cols)
        if s < nz - 1:
            facc[...] += jnp.dot(back[zz], block, preferred_element_type=f32)

    def last_rows(k):
        place = pl.ds(pl.multiple_of(k * own_rows, own_rows), own_rows)
        facc[place, :] += jnp.dot(back[zz, place, :], block, preferred_element_type=f32)

    def finished(k):
        place = pl.ds(pl.multiple_of(k * own_rows, own_rows), own_rows)
        value, signs = facc[place, :], sgn_col[place, :]
        return jnp.concatenate(
            [value[:, j : j + 128] * signs for j in range(0, cols, 128)], axis=1
        ).astype(bf16)

    last_rows(oc)
    f_send[...] = finished(oc)
    f_copy = remote(f_send, f_recv, core_sems.at[0, 5], core_sems.at[1, 5], other)
    f_copy.start()
    last_rows(c)
    full_ref[pl.ds(c, 1)] = finished(c)[None]
    late_pieces()

    f_copy.wait_recv()
    for k, place in enumerate(places):
        g_copy(k, place).wait_recv()
    ig_ref[pl.ds(oc, 1)] = g_recv[...][None]
    full_ref[pl.ds(oc, 1)] = f_recv[...][None]

    for p in range(4):
        tok_copy(p).wait_send()
    for k, place in enumerate(places):
        g_copy(k, place).wait_send()
    for copy in early + res_copies + [f_copy]:
        copy.wait_send()
    for s in range(1, n_t):
        for k in range(2):
            hx_copy(s, k).wait_send()
        hf_copy(s).wait_send()
        for k in range(2 * nb):
            wx_copy(s, k).wait_send()
        for p in range(2):
            wz_copy(s, p).wait_send()
            for dy in y_peers:
                wy_copy(s, p, dy).wait_send()

    def sent(i, carry):
        for dy in y_peers:
            y_copy(i, dy).wait_send()
        for s in tensor_peers:
            x_copy(i, s).wait_send()
        return carry

    def sent_direct(i, carry):
        for dt, dy in corners:
            corner_copy(i, dt, dy).wait_send()
        return carry

    if first_direct:
        lax.fori_loop(0, first_direct, sent, 0)
    lax.fori_loop(first_direct, nz, sent_direct, 0)
    for i in range(nz - 1):
        z_copy(i).wait_send()
    for s in range(nz):
        for dy in range(nb):
            if s or dy:
                ag_copy(s, dy).wait_send()


def write_kernel(ig, nf, ns, full, ig_out, nf_out, ns_out, full_out, sems):
    half = ig.shape[2]
    copies = [(ig.at[k], ig_out.at[:, k * half : (k + 1) * half]) for k in range(2)]
    copies += [(full, full_out), (nf, nf_out), (ns, ns_out)]
    copies = [pltpu.make_async_copy(a, b, sems.at[i]) for i, (a, b) in enumerate(copies)]
    for copy in copies:
        copy.start()
    for copy in copies:
        copy.wait()


def shards(
    tokens, projection_weights, head_cotangent, frequencies, sign_bits, first_moment, second_moment
):
    rows, lw = tokens.shape
    n_t, n_dp = lax.axis_size("tensor"), lax.axis_size("dp")
    width = lw * n_t
    rank = frequencies.shape[1]
    own, cols = first_moment.shape[1], first_moment.shape[2]
    own_rows = projection_weights.shape[1] // n_dp
    chips = n_dp // 2
    cr = 2 * own
    nb = 2
    while nb * cr % 128:
        nb *= 2
    nz = chips // nb
    zr = nb * cr
    low_rows = min(128, 2 * own_rows)
    up8 = lambda n: -(-n // 8) * 8
    half = lw // 2

    anywhere, vmem = pl.BlockSpec(memory_space=pltpu.HBM), pl.BlockSpec(memory_space=pltpu.VMEM)
    dma = pltpu.SemaphoreType.DMA
    V = pltpu.VMEM
    args = (tokens, projection_weights, head_cotangent, frequencies, sign_bits, first_moment, second_moment)
    plan = (n_t, nz, nb, low_rows, rows * n_dp, width)
    ig, nf, ns, full = pl.pallas_call(
        functools.partial(main_kernel, plan),
        out_shape=(
            jax.ShapeDtypeStruct((2, rows, half), bf16),
            jax.ShapeDtypeStruct((2, own, cols), f32),
            jax.ShapeDtypeStruct((2, own, cols), f32),
            jax.ShapeDtypeStruct((2, own_rows, cols), bf16),
        ),
        in_specs=[anywhere] * 7,
        out_specs=(vmem,) * 4,
        scratch_shapes=[
            V((2, rows, lw), bf16), V((2, rows, lw), bf16), V((2, rank), jnp.int32),
            V((2, lw), jnp.int32), V((2, 2 * own_rows), jnp.int32),
            V((nz, low_rows, zr), f32), V((nz, low_rows, zr), f32),
            V((nz, up8(lw // low_rows), zr), f32), V((nz, up8(lw // low_rows), zr), f32),
            V((nz, up8(2 * own_rows // low_rows), zr), f32), V((nz, up8(2 * own_rows // low_rows), zr), f32),
            V((nz, 2 * own_rows, zr), bf16), V((2 * own_rows, 128), f32),
            V((n_t, 2, 2, rows, cols), bf16), V((2 * rows, n_t * cols), bf16), V((n_t, 2 * rows, 2 * cols), bf16),
            V((nz, nb, cr, n_t * cols), bf16), V((nz, nb - 1, cr, n_t * cols), bf16),
            V((nz, n_t, cr, cols), bf16), V((nz, n_t - 1, cr, cols), bf16),
            V((min(DIRECT, nz), n_t * nb - 1, cr, cols), bf16),
            V((nz, cr, cols), bf16), V((nz, cr, cols), bf16),
            V((2, 2, own, cols), f32), V((2, 2, own, cols), f32), V((2, own, cols), f32),
            V((nz * nb, cr, cols), bf16), V((2 * own_rows, cols), f32),
            V((own_rows, cols), bf16), V((own_rows, cols), bf16),
            V((2, half, cols), bf16), V((n_t - 1, 2, half, cols), bf16),
            V((2 * rows, half), f32), V((rows, half), bf16), V((rows, half), bf16),
            dma((8,)), dma((2, 6)), dma((2, 4 * nb)), dma((2, 4)), dma((2, n_t - 1, 2)), dma((2, n_t - 1)),
            dma((2, n_t - 1, 2 * nb)), dma((2, n_t - 1, 2, nb - 1)), dma((2, n_t - 1, 2)),
            dma((2, nz, nb - 1)), dma((2, nz, n_t - 1)),
            dma((2, min(DIRECT, nz), n_t * nb - 1)), dma((2, nz)), dma((2, nz, nb)),
        ],
        compiler_params=pltpu.CompilerParams(
            collective_id=0, has_side_effects=True, vmem_limit_bytes=48 * 1024 * 1024
        ),
    )(*(pltpu.with_memory_space_constraint(a, pltpu.HBM) for a in args))
    return pl.pallas_call(
        write_kernel,
        out_shape=(
            jax.ShapeDtypeStruct((rows, lw), bf16),
            jax.ShapeDtypeStruct((2, own, cols), f32),
            jax.ShapeDtypeStruct((2, own, cols), f32),
            jax.ShapeDtypeStruct((2, own_rows, cols), bf16),
        ),
        in_specs=[vmem] * 4,
        out_specs=(anywhere,) * 4,
        scratch_shapes=[dma((5,))],
        compiler_params=pltpu.CompilerParams(vmem_limit_bytes=8 * 1024 * 1024),
    )(ig, nf, ns, full)


def solution(mesh):
    in_specs = (
        P("dp", "tensor"),
        P(None, None, "tensor"),
        P(None, "dp", "tensor"),
        P(),
        P(),
        P(None, "dp", "tensor"),
        P(None, "dp", "tensor"),
    )
    out_specs = (
        P("dp", "tensor"),
        P(None, "dp", "tensor"),
        P(None, "dp", "tensor"),
        P(None, "dp", "tensor"),
    )
    return jax.shard_map(shards, mesh=mesh, in_specs=in_specs, out_specs=out_specs, check_vma=False)
```
